8 devices in a mesh: dp: 2 (over y, z), ep: 4 (over x, core).
Axes of the slice: x: 2, y: 2, z: 1, core: 2. Of those that a mesh axis runs over, the one named last changes fastest.
Arguments:
- x: bfloat16 [2, 4, 256, 3584], P('dp', 'ep'), parts along dimension 0
- expert: int32 [2, 4, 256, 8], P('dp', 'ep'), parts along dimension 0
- slot: int32 [2, 4, 256, 8], P('dp', 'ep'), parts along dimension 0
- gate: float32 [2, 4, 256, 8], P('dp', 'ep'), parts along dimension 0
- w_gate: bfloat16 [32, 3584, 2560], P('ep')
- w_up: bfloat16 [32, 3584, 2560], P('ep')
- w_down: bfloat16 [32, 2560, 3584], P('ep')
- s_gate: bfloat16 [3584, 20480], replicated
- s_up: bfloat16 [3584, 20480], replicated
- s_down: bfloat16 [20480, 3584], replicated
Outputs:
- y: bfloat16 [2, 4, 256, 3584], P('dp', 'ep'), parts along dimension 0
There are 2 independent parts. The reference program is written for one: setup_inputs(seed, part) draws one part's arguments, and reference() takes and returns one part's arrays. A program takes and returns all parts, laid end to end along the dimension named above; an argument that names none is the same for every part.
All inputs are finite; a program needn't handle non-finite values.
Results may differ from the reference program's by a relative error of at most 0.009.
Values are sent between devices in bfloat16 or wider.
A program may use at most 2.25 GiB of HBM per device.

```python
import jax
import jax.numpy as jnp

MEMBERS = 4
TOKENS = 256
D = 3584
FF = 2560
TOP = 8
EXPERTS = 32
SHARED_FF = 20480
SLOTS = 5 * TOKENS * TOP // (4 * EXPERTS)


def setup_inputs(seed: int = 0, part: int = 0) -> dict:
    own, k1, k2, k3, k4, k5, k6 = jax.random.split(jax.random.key(seed), 7)
    kx, ke, kl, kg = jax.random.split(jax.random.fold_in(own, part), 4)
    devices = (1, MEMBERS)
    place = jax.random.permutation(kl, jnp.arange(EXPERTS, dtype=jnp.uint32))
    slow = ((EXPERTS + (9 * place) % EXPERTS) << ((9 * place) // EXPERTS)) // EXPERTS
    wait = (jax.random.bits(ke, (*devices, TOKENS, EXPERTS), jnp.uint32) >> 10) * slow
    expert = jnp.argsort(wait, axis=-1)[..., :TOP].astype(jnp.int32)
    chosen = jax.nn.one_hot(expert, EXPERTS, dtype=jnp.int32)
    in_line = jnp.cumsum(chosen.reshape(*devices, TOKENS * TOP, EXPERTS), axis=2) - 1
    slot = jnp.sum(in_line.reshape(chosen.shape) * chosen, axis=-1)

    def one(key, rows, columns):
        return (jax.random.normal(key, (rows, columns), jnp.float32) * rows**-0.5).astype(jnp.bfloat16)

    def weights(key, rows, columns):
        return jax.lax.map(lambda k: one(k, rows, columns), jax.random.split(key, EXPERTS))

    return {
        "x": jax.random.normal(kx, (*devices, TOKENS, D), jnp.float32).astype(jnp.bfloat16),
        "expert": expert,
        "slot": slot,
        "gate": jax.nn.softmax(jax.random.normal(kg, expert.shape, jnp.float32)),
        "w_gate": weights(k1, D, FF),
        "w_up": weights(k2, D, FF),
        "w_down": weights(k3, FF, D),
        "s_gate": one(k4, D, SHARED_FF),
        "s_up": one(k5, D, SHARED_FF),
        "s_down": one(k6, SHARED_FF, D),
    }


def einsum(form, a, b):
    return jnp.einsum(form, a.astype(jnp.float32), b.astype(jnp.float32))


def for_all(x, s_gate, s_up, s_down):
    h = jax.nn.silu(einsum("...d,df->...f", x, s_gate)) * einsum("...d,df->...f", x, s_up)
    return einsum("...f,fd->...d", h.astype(jnp.bfloat16), s_down)


def reference(x, expert, slot, gate, w_gate, w_up, w_down, s_gate, s_up, s_down):
    to_expert = jax.nn.one_hot(expert, EXPERTS, dtype=jnp.bfloat16)
    to_slot = jax.nn.one_hot(slot, SLOTS, dtype=jnp.bfloat16)
    weighted = to_expert * gate[..., None].astype(jnp.bfloat16)
    dispatch = einsum("abtke,abtkc->abtec", to_expert, to_slot).astype(jnp.bfloat16)
    combine = einsum("abtke,abtkc->abtec", weighted, to_slot).astype(jnp.bfloat16)
    z = einsum("abtec,abtd->aebcd", dispatch, x).astype(jnp.bfloat16)
    h = jax.nn.silu(einsum("aebcd,edf->aebcf", z, w_gate))
    h = (h * einsum("aebcd,edf->aebcf", z, w_up)).astype(jnp.bfloat16)
    out = einsum("aebcf,efd->aebcd", h, w_down).astype(jnp.bfloat16)
    y = einsum("abtec,aebcd->abtd", combine, out)
    return (y + for_all(x, s_gate, s_up, s_down)).astype(jnp.bfloat16)
```

```python
import functools

import jax
import jax.numpy as jnp
from jax import lax
from jax.experimental import pallas as pl
from jax.experimental.pallas import tpu as pltpu
from jax.sharding import PartitionSpec as P


CHUNK = 16
VMEM_LIMIT = 66_000_000


def dot(a, b):
    return jnp.dot(a, b, preferred_element_type=jnp.float32)


def swiglu(g, u):
    return (g * jax.nn.sigmoid(g) * u).astype(jnp.bfloat16)


def shared_call(x2, off, sg, su, sd, first, blocks, bf, init=None, name="shared"):
    m, d = x2.shape
    half = m // 2
    last = init is not None

    def kern(off_ref, x_ref, g_ref, u_ref, d_ref, *rest):
        i = pl.program_id(0)
        if last:
            init_ref, own_ref, sib_ref, acc, sem = rest
        else:
            out_ref, acc = rest

        @pl.when(i == 0)
        def _():
            if last:
                copy = pltpu.make_async_copy(init_ref, acc, sem)
                copy.start()
                copy.wait()
            else:
                acc[...] = jnp.zeros_like(acc)

        g = dot(x_ref[...], g_ref[...])
        u = dot(x_ref[...], u_ref[...])
        acc[...] += dot(swiglu(g, u), d_ref[...])

        @pl.when(i == blocks - 1)
        def _():
            if last:
                own_ref[...] = acc[:half]
                sib_ref[...] = acc[half:]
            else:
                out_ref[...] = acc[...]

    in_specs = [
        pl.BlockSpec((m, d), lambda i, o: (0, 0)),
        pl.BlockSpec((d, bf), lambda i, o: (0, o[0] + first + i)),
        pl.BlockSpec((d, bf), lambda i, o: (0, o[0] + first + i)),
        pl.BlockSpec((bf, d), lambda i, o: (o[0] + first + i, 0)),
    ]
    args = [off, x2, sg, su, sd]
    scratch = [pltpu.VMEM((m, d), jnp.float32)]
    if last:
        in_specs.append(pl.BlockSpec(memory_space=pl.ANY))
        args.append(init)
        scratch.append(pltpu.SemaphoreType.DMA)
        out_shape = [jax.ShapeDtypeStruct((half, d), jnp.float32)] * 2
        out_specs = [pl.BlockSpec((half, d), lambda i, o: (0, 0))] * 2
    else:
        out_shape = jax.ShapeDtypeStruct((m, d), jnp.float32)
        out_specs = pl.BlockSpec((m, d), lambda i, o: (0, 0))
    return pl.pallas_call(
        kern,
        out_shape=out_shape,
        grid_spec=pltpu.PrefetchScalarGridSpec(
            num_scalar_prefetch=1,
            grid=(blocks,),
            in_specs=in_specs,
            out_specs=out_specs,
            scratch_shapes=scratch,
        ),
        compiler_params=pltpu.CompilerParams(
            vmem_limit_bytes=VMEM_LIMIT, dimension_semantics=("arbitrary",)
        ),
        cost_estimate=pl.CostEstimate(
            flops=6 * m * d * bf * blocks,
            bytes_accessed=6 * d * bf * blocks,
            transcendentals=m * bf * blocks,
        ),
        name=name,
    )(*args)


def routed_call(xs, codes, eoff, wg, wu, wd, experts, slots, bf):
    n_src = len(xs)
    groups = n_src // 4
    tokens, d = xs[0].shape
    ff = wg.shape[2]
    nf = ff // bf
    chunks = slots // CHUNK
    top = codes.shape[1]

    def kern(eoff_ref, code_ref, *rest):
        x_refs = rest[:n_src]
        g_ref, u_ref, d_ref, out_ref, z, acc, used = rest[n_src:]
        e, f = pl.program_id(0), pl.program_id(1)

        @pl.when(f == 0)
        def _():
            low = (e * slots).astype(jnp.float32)
            row = low + lax.broadcasted_iota(jnp.int32, (slots, tokens), 0).astype(jnp.float32)
            for grp in range(groups):
                most = jnp.full((top, tokens), -1.0, jnp.float32)
                for k in range(4):
                    s = grp * 4 + k
                    code = code_ref[s]
                    here = (code >= low) & (code < low + slots)
                    most = jnp.maximum(most, jnp.where(here, code - low, -1.0))
                    pick = jnp.zeros((slots, tokens), jnp.float32)
                    for j in range(top):
                        pick = jnp.where(row == code[j : j + 1, :], 1.0, pick)
                    zs = dot(pick.astype(jnp.bfloat16), x_refs[s][...]).astype(jnp.bfloat16)
                    z[grp, :, k] = zs.reshape(chunks, CHUNK, d)
                used[grp] = (jnp.max(most).astype(jnp.int32) + CHUNK) // CHUNK
            acc[...] = jnp.zeros_like(acc)

        for grp in range(groups):
            for v in range(1, chunks + 1):

                @pl.when(used[grp] == v)
                def _(grp=grp, v=v):
                    m = v * 4 * CHUNK
                    zz = z[grp, :v].reshape(m, d)
                    h = swiglu(dot(zz, g_ref[0]), dot(zz, u_ref[0]))
                    acc[grp, :m] += dot(h, d_ref[0])

        @pl.when(f == nf - 1)
        def _():
            out_ref[0] = acc[...].astype(jnp.bfloat16).reshape(groups, chunks, 4, CHUNK, d)

    rows = chunks * 4 * CHUNK
    total = experts * groups * rows
    return pl.pallas_call(
        kern,
        out_shape=jax.ShapeDtypeStruct((experts, groups, chunks, 4, CHUNK, d), jnp.bfloat16),
        grid_spec=pltpu.PrefetchScalarGridSpec(
            num_scalar_prefetch=1,
            grid=(experts, nf),
            in_specs=[pl.BlockSpec((n_src, top, tokens), lambda e, f, o: (0, 0, 0))]
            + [
                pl.BlockSpec((tokens, d), lambda e, f, o: (0, 0), pipeline_mode=pl.Buffered(1))
            ]
            * n_src
            + [
                pl.BlockSpec((1, d, bf), lambda e, f, o: (o[0] + e, 0, f)),
                pl.BlockSpec((1, d, bf), lambda e, f, o: (o[0] + e, 0, f)),
                pl.BlockSpec((1, bf, d), lambda e, f, o: (o[0] + e, f, 0)),
            ],
            out_specs=pl.BlockSpec(
                (1, groups, chunks, 4, CHUNK, d), lambda e, f, o: (e, 0, 0, 0, 0, 0)
            ),
            scratch_shapes=[
                pltpu.VMEM((groups, chunks, 4, CHUNK, d), jnp.bfloat16),
                pltpu.VMEM((groups, rows, d), jnp.float32),
                pltpu.SMEM((groups,), jnp.int32),
            ],
        ),
        compiler_params=pltpu.CompilerParams(
            vmem_limit_bytes=VMEM_LIMIT, dimension_semantics=("arbitrary", "arbitrary")
        ),
        cost_estimate=pl.CostEstimate(
            flops=6 * total * d * ff,
            bytes_accessed=6 * experts * d * ff,
            transcendentals=total * ff,
        ),
        name="routed",
    )(eoff, codes, *xs, wg, wu, wd)


def combine_call(out, codes, gates, sources, types, adds, slots, name):
    experts, groups, chunks, _, _, d = out.shape
    top, tokens = codes.shape[1:]
    n = len(sources)

    def kern(code_ref, gate_ref, *rest):
        out_refs, add_refs, y_refs = rest[:n], rest[n : n + len(adds)], rest[n + len(adds) :]
        row = lax.broadcasted_iota(jnp.int32, (experts * slots, tokens), 0).astype(jnp.float32)
        for i, s in enumerate(sources):
            weight = jnp.zeros((experts * slots, tokens), jnp.float32)
            for j in range(top):
                weight = jnp.where(
                    row == code_ref[s, j : j + 1, :], gate_ref[s, j : j + 1, :], weight
                )
            o = out_refs[i][...].reshape(experts * slots, -1)
            y = lax.dot_general(
                weight.astype(jnp.bfloat16),
                o,
                (((0,), (0,)), ((), ())),
                preferred_element_type=jnp.float32,
            )
            if adds:
                y = y + add_refs[i][...]
            y_refs[i][...] = y.astype(types[i])

    bn = 512
    return pl.pallas_call(
        kern,
        out_shape=[jax.ShapeDtypeStruct((tokens, d), t) for t in types],
        grid=(d // bn,),
        in_specs=[pl.BlockSpec(codes.shape, lambda n: (0, 0, 0))] * 2
        + [
            pl.BlockSpec(
                (experts, 1, chunks, 1, CHUNK, bn),
                lambda n, s=s: (0, s // 4, 0, s % 4, 0, n),
            )
            for s in sources
        ]
        + [
            pl.BlockSpec((tokens, bn), lambda n, a=a: (a[1], n)) for a in adds
        ],
        out_specs=[pl.BlockSpec((tokens, bn), lambda n: (0, n))] * n,
        compiler_params=pltpu.CompilerParams(
            vmem_limit_bytes=VMEM_LIMIT, dimension_semantics=("arbitrary",)
        ),
        cost_estimate=pl.CostEstimate(
            flops=2 * n * tokens * experts * slots * d,
            bytes_accessed=2 * n * experts * slots * d,
            transcendentals=0,
        ),
        name=name,
    )(codes, gates, *([out] * n), *[a[0] for a in adds])


def solution(mesh):
    def body(x, expert, slot, gate, wg, wu, wd, sg, su, sd):
        x = x[0, 0]
        top, experts, ff = expert.shape[-1], wg.shape[0], sg.shape[1]
        tokens = x.shape[0]
        slots = 5 * tokens * top // (4 * experts * 4)
        me = lax.axis_index("ep")

        def swap(v, bit):
            return lax.ppermute(v, "ep", [(i, i ^ bit) for i in range(4)])

        code = jnp.where(slot < slots, expert * slots + slot, -1)[0, 0]
        weight = gate[0, 0].astype(jnp.bfloat16).astype(jnp.float32)
        small = jnp.stack([code.astype(jnp.float32).T, weight.T])
        x_nb = swap(x, 2)
        x_sib = swap(x, 1)
        smalls = jnp.stack([small] + [swap(small, bit) for bit in (1, 2, 3)])
        codes = smalls[:, 0] - (me * experts * slots).astype(jnp.float32)
        gates = smalls[:, 1]

        bf = 512
        blocks = ff // 2 // bf
        lead = blocks // 2
        off = jnp.reshape((me % 2) * blocks, (1,)).astype(jnp.int32)
        x2 = jnp.concatenate([x, x_sib])
        acc = shared_call(x2, off, sg, su, sd, 0, lead, bf, name="shared_a")
        x_diag = swap(x_nb, 1)

        eoff = jnp.zeros((1,), jnp.int32)
        out = routed_call([x, x_sib, x_nb, x_diag], codes, eoff, wg, wu, wd, experts, slots, 512)
        far, far_sib = combine_call(
            out, codes, gates, (2, 3), (jnp.float32, jnp.bfloat16), (), slots, "combine_far"
        )
        far = (far + swap(far_sib, 1).astype(jnp.float32)).astype(jnp.bfloat16)
        far = swap(far, 2)
        own, sib = shared_call(
            x2, off, sg, su, sd, lead, blocks - lead, bf, init=acc, name="shared_b"
        )
        own, sib = combine_call(
            out,
            codes,
            gates,
            (0, 1),
            (jnp.float32, jnp.bfloat16),
            ((own, 0), (sib, 0)),
            slots,
            "combine_near",
        )
        y = own + swap(sib, 1).astype(jnp.float32) + far.astype(jnp.float32)
        return y.astype(jnp.bfloat16)[None, None]

    lead = P("dp", "ep", None, None)
    return jax.shard_map(
        body,
        mesh=mesh,
        in_specs=(lead,) * 4 + (P("ep", None, None),) * 3 + (P(None, None),) * 3,
        out_specs=lead,
        check_vma=False,
    )
```

```python
import jax
import jax.numpy as jnp
from jax import lax
from jax.experimental import pallas as pl
from jax.experimental.pallas import tpu as pltpu
from jax.sharding import PartitionSpec as P


CHUNK = 16
VMEM_LIMIT = 66_500_000
X, Y, CORE = 2, 4, 1


def dot(a, b):
    return jnp.dot(a, b, preferred_element_type=jnp.float32)


def swiglu(g, u):
    return (g * jax.nn.sigmoid(g) * u).astype(jnp.bfloat16)


def params(n):
    return pltpu.CompilerParams(
        vmem_limit_bytes=VMEM_LIMIT, dimension_semantics=("arbitrary",) * n
    )


def shared_up(xa, xb, off, sg, su, first, blocks, bf, name):
    half, d = xa.shape

    def kern(off_ref, xa_ref, xb_ref, g_ref, u_ref, h_ref, x, sems):
        @pl.when(pl.program_id(0) == 0)
        def _():
            a = pltpu.make_async_copy(xa_ref, x.at[:half], sems.at[0])
            b = pltpu.make_async_copy(xb_ref, x.at[half:], sems.at[1])
            a.start()
            b.start()
            a.wait()
            b.wait()

        h_ref[...] = swiglu(dot(x[...], g_ref[...]), dot(x[...], u_ref[...]))

    return pl.pallas_call(
        kern,
        out_shape=jax.ShapeDtypeStruct((2 * half, blocks * bf), jnp.bfloat16),
        grid_spec=pltpu.PrefetchScalarGridSpec(
            num_scalar_prefetch=1,
            grid=(blocks,),
            in_specs=[pl.BlockSpec(memory_space=pl.ANY)] * 2
            + [pl.BlockSpec((d, bf), lambda i, o: (0, o[0] + first + i))] * 2,
            out_specs=pl.BlockSpec((2 * half, bf), lambda i, o: (0, i)),
            scratch_shapes=[
                pltpu.VMEM((2 * half, d), jnp.bfloat16),
                pltpu.SemaphoreType.DMA((2,)),
            ],
        ),
        compiler_params=params(1),
        cost_estimate=pl.CostEstimate(
            flops=8 * half * d * bf * blocks,
            bytes_accessed=4 * d * bf * blocks,
            transcendentals=2 * half * bf * blocks,
        ),
        name=name,
    )(off, xa, xb, sg, su)


def shared_down(hs, inits, off, sd, bf, name):
    m, d = hs[0].shape[0], sd.shape[1]
    half = m // 2
    counts = [h.shape[1] // bf for h in hs]
    starts = [sum(counts[:i]) for i in range(len(hs))]
    blocks = sum(counts)

    def kern(off_ref, *rest):
        h_refs = rest[: len(hs)]
        d_ref, ia_ref, ib_ref, own_ref, sib_ref, acc, sems = rest[len(hs) :]
        i = pl.program_id(0)

        @pl.when(i == 0)
        def _():
            a = pltpu.make_async_copy(ia_ref, acc.at[:half], sems.at[0])
            b = pltpu.make_async_copy(ib_ref, acc.at[half:], sems.at[1])
            a.start()
            b.start()
            a.wait()
            b.wait()

        for h_ref, start, count in zip(h_refs, starts, counts):

            @pl.when((i >= start) & (i < start + count))
            def _(h_ref=h_ref):
                acc[...] += dot(h_ref[...], d_ref[...])

        @pl.when(i == blocks - 1)
        def _():
            own_ref[...] = acc[:half]
            sib_ref[...] = acc[half:].astype(jnp.bfloat16)

    return pl.pallas_call(
        kern,
        out_shape=[
            jax.ShapeDtypeStruct((half, d), jnp.float32),
            jax.ShapeDtypeStruct((half, d), jnp.bfloat16),
        ],
        grid_spec=pltpu.PrefetchScalarGridSpec(
            num_scalar_prefetch=1,
            grid=(blocks,),
            in_specs=[
                pl.BlockSpec((m, bf), lambda i, o, s=s, c=c: (0, jnp.clip(i - s, 0, c - 1)))
                for s, c in zip(starts, counts)
            ]
            + [pl.BlockSpec((bf, d), lambda i, o: (o[0] + i, 0))]
            + [pl.BlockSpec(memory_space=pl.ANY)] * 2,
            out_specs=[pl.BlockSpec((half, d), lambda i, o: (0, 0))] * 2,
            scratch_shapes=[
                pltpu.VMEM((m, d), jnp.float32),
                pltpu.SemaphoreType.DMA((2,)),
            ],
        ),
        compiler_params=params(1),
        cost_estimate=pl.CostEstimate(
            flops=2 * m * d * bf * blocks,
            bytes_accessed=2 * d * bf * blocks,
            transcendentals=0,
        ),
        name=name,
    )(off, *hs, sd, *inits)


def routed_call(xs, codes, eoff, wg, wu, wd, experts, slots, bf):
    n_src = len(xs)
    flat = [piece for pieces in xs for piece in pieces]
    groups = n_src // 4
    d = flat[0].shape[1]
    ff = wg.shape[2]
    nf = ff // bf
    chunks = slots // CHUNK
    top, tokens = codes.shape[1:]

    def kern(eoff_ref, code_ref, *rest):
        x_refs = list(rest[: len(flat)])
        g_ref, u_ref, d_ref, out_ref, z, acc, used = rest[len(flat) :]
        e, f = pl.program_id(0), pl.program_id(1)

        @pl.when(f == 0)
        def _():
            low = (e * slots).astype(jnp.float32)
            row = low + lax.broadcasted_iota(jnp.int32, (slots, tokens), 0).astype(jnp.float32)
            at = 0
            for grp in range(groups):
                most = jnp.full((top, tokens), -1.0, jnp.float32)
                for k in range(4):
                    s = grp * 4 + k
                    code = code_ref[s]
                    here = (code >= low) & (code < low + slots)
                    most = jnp.maximum(most, jnp.where(here, code - low, -1.0))
                    pick = jnp.zeros((slots, tokens), jnp.float32)
                    for j in range(top):
                        pick = jnp.where(row == code[j : j + 1, :], 1.0, pick)
                    pick = pick.astype(jnp.bfloat16)
                    zs, t = None, 0
                    for _ in xs[s]:
                        n = flat[at].shape[0]
                        part = dot(pick[:, t : t + n], x_refs[at][...])
                        zs = part if zs is None else zs + part
                        at, t = at + 1, t + n
                    z[grp, :, k] = zs.astype(jnp.bfloat16).reshape(chunks, CHUNK, d)
                used[grp] = (jnp.max(most).astype(jnp.int32) + CHUNK) // CHUNK
            acc[...] = jnp.zeros_like(acc)

        for grp in range(groups):
            for v in range(1, chunks + 1):

                @pl.when(used[grp] == v)
                def _(grp=grp, v=v):
                    m = v * 4 * CHUNK
                    zz = z[grp, :v].reshape(m, d)
                    h = swiglu(dot(zz, g_ref[0]), dot(zz, u_ref[0]))
                    acc[grp, :m] += dot(h, d_ref[0])

        @pl.when(f == nf - 1)
        def _():
            out_ref[0] = acc[...].astype(jnp.bfloat16).reshape(groups, chunks, 4, CHUNK, d)

    rows = chunks * 4 * CHUNK
    total = experts * groups * rows
    return pl.pallas_call(
        kern,
        out_shape=jax.ShapeDtypeStruct((experts, groups, chunks, 4, CHUNK, d), jnp.bfloat16),
        grid_spec=pltpu.PrefetchScalarGridSpec(
            num_scalar_prefetch=1,
            grid=(experts, nf),
            in_specs=[pl.BlockSpec(codes.shape, lambda e, f, o: (0, 0, 0))]
            + [
                pl.BlockSpec(v.shape, lambda e, f, o: (0, 0), pipeline_mode=pl.Buffered(1))
                for v in flat
            ]
            + [
                pl.BlockSpec((1, d, bf), lambda e, f, o: (o[0] + e, 0, f)),
                pl.BlockSpec((1, d, bf), lambda e, f, o: (o[0] + e, 0, f)),
                pl.BlockSpec((1, bf, d), lambda e, f, o: (o[0] + e, f, 0)),
            ],
            out_specs=pl.BlockSpec(
                (1, groups, chunks, 4, CHUNK, d), lambda e, f, o: (e, 0, 0, 0, 0, 0)
            ),
            scratch_shapes=[
                pltpu.VMEM((groups, chunks, 4, CHUNK, d), jnp.bfloat16),
                pltpu.VMEM((groups, rows, d), jnp.float32),
                pltpu.SMEM((groups,), jnp.int32),
            ],
        ),
        compiler_params=params(2),
        cost_estimate=pl.CostEstimate(
            flops=4 * total * d * ff,
            bytes_accessed=6 * experts * d * ff,
            transcendentals=total * ff,
        ),
        name="routed",
    )(eoff, codes, *flat, wg, wu, wd)


def combine_call(out, codes, gates, sources, types, adds, slots, name):
    experts, groups, chunks, _, _, d = out.shape
    top, tokens = codes.shape[1:]
    n = len(sources)
    flat = [a for part in adds for a, _ in part]
    bn = 512

    def kern(code_ref, gate_ref, *rest):
        out_refs, add_refs = rest[:n], list(rest[n : n + len(flat)])
        y_refs, weights = rest[n + len(flat) : -1], rest[-1]

        @pl.when(pl.program_id(0) == 0)
        def _():
            row = lax.broadcasted_iota(jnp.int32, (experts * slots, tokens), 0)
            row = row.astype(jnp.float32)
            for i, s in enumerate(sources):
                weight = jnp.zeros(row.shape, jnp.float32)
                for j in range(top):
                    weight = jnp.where(
                        row == code_ref[s, j : j + 1, :], gate_ref[s, j : j + 1, :], weight
                    )
                weights[i] = weight.T.astype(jnp.bfloat16)

        at = 0
        for i in range(n):
            y = dot(weights[i], out_refs[i][...].reshape(experts * slots, bn))
            if not adds or not adds[i]:
                y_refs[i][...] = y.astype(types[i])
                continue
            parts = [y]
            for a, first in adds[i]:
                m, v = a.shape[0], add_refs[at][...].astype(jnp.float32)
                at += 1
                if m < tokens:
                    zero = jnp.zeros((tokens - m, bn), jnp.float32)
                    v = jnp.concatenate([v, zero] if first == 0 else [zero, v])
                parts.append(v)
            y_refs[i][...] = sum(parts).astype(types[i])

    return pl.pallas_call(
        kern,
        out_shape=[jax.ShapeDtypeStruct((tokens, d), t) for t in types],
        grid=(d // bn,),
        in_specs=[pl.BlockSpec(codes.shape, lambda n: (0, 0, 0))] * 2
        + [
            pl.BlockSpec(
                (experts, 1, chunks, 1, CHUNK, bn),
                lambda n, s=s: (0, s // 4, 0, s % 4, 0, n),
            )
            for s in sources
        ]
        + [pl.BlockSpec((a.shape[0], bn), lambda n: (0, n)) for a in flat],
        out_specs=[pl.BlockSpec((tokens, bn), lambda n: (0, n))] * n,
        scratch_shapes=[pltpu.VMEM((n, tokens, experts * slots), jnp.bfloat16)],
        compiler_params=params(1),
        cost_estimate=pl.CostEstimate(
            flops=2 * n * tokens * experts * slots * d,
            bytes_accessed=2 * n * experts * slots * d,
            transcendentals=0,
        ),
        name=name,
    )(codes, gates, *([out] * n), *flat)


def solution(mesh):
    groups = mesh.shape["dp"]

    def swap(v, bit):
        return lax.ppermute(v, ("dp", "ep"), [(i, i ^ bit) for i in range(8)])

    after = lax.optimization_barrier

    def body(x, expert, slot, gate, wg, wu, wd, sg, su, sd):
        x = x[0, 0]
        tokens, d = x.shape
        half = tokens // 2
        top, ff = expert.shape[-1], sg.shape[1]
        slots = 5 * tokens * top // (4 * wg.shape[0] * mesh.shape["ep"])
        experts = wg.shape[0] // groups
        me, part = lax.axis_index("ep"), lax.axis_index("dp")
        bf = 512
        blocks = ff // 2 // bf
        one, two = 9, 5
        off = jnp.reshape((me % 2) * blocks, (1,)).astype(jnp.int32)
        eoff = jnp.reshape(part * experts, (1,)).astype(jnp.int32)

        code = jnp.where(slot < slots, expert * slots + slot, -1)[0, 0]
        weight = gate[0, 0].astype(jnp.bfloat16).astype(jnp.float32)
        small = jnp.stack([code.astype(jnp.float32).T, weight.T])
        xc = swap(x, CORE)
        smalls = [small] + [swap(small, bit) for bit in range(1, 8)]
        xx = swap(x, X)
        xy = swap(x, Y)

        h1 = shared_up(x, xc, off, sg, su, 0, one, bf, "up_1")
        h1, xx, xy, xa, xb, *smalls = after((h1, xx, xy, x, xc, *smalls))
        xxy = [swap(xy[:half], X), swap(xx[half:], Y)]
        xxc, xyc = swap(xx, CORE), swap(xy, CORE)
        h2 = shared_up(xa, xb, off, sg, su, one, two, bf, "up_2")
        h2, xxc, xyc, t, b, *smalls = after((h2, xxc, xyc, *xxy, *smalls))
        xxyc = [swap(t, CORE), swap(b, CORE)]
        smalls = jnp.stack(smalls)
        base = (me * wg.shape[0] + part * experts) * slots
        codes = smalls[:, 0] - base.astype(jnp.float32)
        gates = smalls[:, 1]

        sources = [[xa], [xb], [xx], [xxc], [xy], [xyc], [t, b], xxyc]
        out = routed_call(sources, codes, eoff, wg, wu, wd, experts, slots, 512)

        f32, bf16 = jnp.float32, jnp.bfloat16

        def combine(sources, types, adds, name):
            return combine_call(out, codes, gates, sources, types, adds, slots, name)

        cx, cy, cxy = combine((3, 5, 7), (bf16,) * 3, (), "combine_core")
        cxy = swap(cxy, CORE)
        cx, cy = swap(cx, CORE), swap(cy, CORE)
        near = combine((0, 1), (f32,) * 2, (), "combine_near")
        (qxy,) = combine((6,), (bf16,), [[(cxy, 0)]], "combine_far")
        qxy, xa, xb = after((qxy, xa, xb))
        t, b = swap(qxy[:half], Y), swap(qxy[half:], X)
        h3 = shared_up(xa, xb, off, sg, su, one + two, blocks - one - two, bf, "up_3")
        h3, t, b = after((h3, t, b))
        qx, qy = combine(
            (2, 4), (bf16,) * 2, [[(cx, 0), (t, 0)], [(cy, 0), (b, half)]], "combine_mid"
        )
        h3, qx, qy = after((h3, qx, qy))
        qx, qy = swap(qx, X), swap(qy, Y)
        own, sib = shared_down([h1, h2, h3], near, off, sd, bf, "down")
        own, sib, qx, qy = after((own, sib, qx, qy))
        y = own + swap(sib, CORE).astype(f32) + qx.astype(f32) + qy.astype(f32)
        return y.astype(bf16)[None, None]

    lead = P("dp", "ep", None, None)
    return jax.shard_map(
        body,
        mesh=mesh,
        in_specs=(lead,) * 4 + (P("ep", None, None),) * 3 + (P(None, None),) * 3,
        out_specs=lead,
        check_vma=False,
    )
```

```python
import jax
import jax.numpy as jnp
from jax import lax
from jax.experimental import pallas as pl
from jax.experimental.pallas import tpu as pltpu
from jax.sharding import PartitionSpec as P


CHUNK = 16
VMEM_LIMIT = 66_500_000
X, Y, CORE = 2, 4, 1


def dot(a, b):
    return jnp.dot(a, b, preferred_element_type=jnp.float32)


def swiglu(g, u):
    return (g * jax.nn.sigmoid(g) * u).astype(jnp.bfloat16)


def params(n):
    return pltpu.CompilerParams(
        vmem_limit_bytes=VMEM_LIMIT, dimension_semantics=("arbitrary",) * n
    )


def place():
    ep = lax.axis_index("ep")
    return lax.axis_index("dp"), ep // 2, ep % 2


def peer(bits):
    y, x, core = place()
    y = 1 - y if bits & Y else y
    x = 1 - x if bits & X else x
    core = 1 - core if bits & CORE else core
    return (y, x * 2 + core)


def gather_up(x, small, sg, su, per_core, blocks, relay, bf):
    tokens, d = x.shape
    half = tokens // 2

    def kern(x_ref, small_ref, g_ref, u_ref, h_ref, all_x, all_small, x2, local, send, recv):
        i = pl.program_id(0)

        def copy(n, src, dst, bits):
            return pltpu.make_async_remote_copy(
                src_ref=src,
                dst_ref=dst,
                send_sem=send.at[n],
                recv_sem=recv.at[n],
                device_id=peer(bits),
                device_id_type=pl.DeviceIdType.MESH,
            )

        def at(bits):
            return all_x.at[bits - 1]

        top, bottom = pl.ds(0, half), pl.ds(half, half)
        first = [copy(n, x_ref, at(b), b) for n, b in enumerate((CORE, X, Y))]
        second = [
            copy(3, at(Y).at[top], at(X | Y).at[top], X),
            copy(4, at(X).at[bottom], at(X | Y).at[bottom], Y),
            copy(5, at(X), at(X | CORE), CORE),
            copy(6, at(Y), at(Y | CORE), CORE),
        ]
        third = [copy(7, at(X | Y), at(X | Y | CORE), CORE)]
        little = [copy(7 + b, small_ref, all_small.at[b - 1], b) for b in range(1, 8)]

        def up(v):
            return swiglu(dot(v, g_ref[...]), dot(v, u_ref[...]))

        @pl.when(i == 0)
        def _():
            own = pltpu.make_async_copy(x_ref, x2.at[pl.ds(0, tokens)], local.at[0])
            own.start()
            barrier = pltpu.get_barrier_semaphore()
            for bits in range(1, 8):
                pl.semaphore_signal(
                    barrier, inc=1, device_id=peer(bits), device_id_type=pl.DeviceIdType.MESH
                )
            pl.semaphore_wait(barrier, 7)
            for c in little + first:
                c.start()
            own.wait()
            h_ref[:tokens] = up(x2[:tokens])
            first[0].wait_recv()
            other = pltpu.make_async_copy(at(CORE), x2.at[pl.ds(tokens, tokens)], local.at[1])
            other.start()
            other.wait()
            h_ref[tokens:] = up(x2[tokens:])

        @pl.when(i == relay)
        def _():
            first[1].wait_recv()
            first[2].wait_recv()
            for c in second:
                c.start()

        @pl.when(i > 0)
        def _():
            h_ref[...] = up(x2[...])

        @pl.when(i == blocks - 1)
        def _():
            second[0].wait_recv()
            second[1].wait_recv()
            third[0].start()
            second[2].wait_recv()
            second[3].wait_recv()
            for c in little:
                c.wait_recv()
            third[0].wait_recv()
            for c in first + second + third + little:
                c.wait_send()

    def column(i):
        return (0, (lax.axis_index("ep") % 2) * per_core + i)

    any_spec = pl.BlockSpec(memory_space=pl.ANY)
    return pl.pallas_call(
        kern,
        out_shape=[
            jax.ShapeDtypeStruct((2 * tokens, blocks * bf), jnp.bfloat16),
            jax.ShapeDtypeStruct((7, tokens, d), x.dtype),
            jax.ShapeDtypeStruct((7, *small.shape), small.dtype),
        ],
        grid=(blocks,),
        in_specs=[any_spec] * 2 + [pl.BlockSpec((d, bf), column)] * 2,
        out_specs=[pl.BlockSpec((2 * tokens, bf), lambda i: (0, i)), any_spec, any_spec],
        scratch_shapes=[
            pltpu.VMEM((2 * tokens, d), jnp.bfloat16),
            pltpu.SemaphoreType.DMA((2,)),
            pltpu.SemaphoreType.DMA((15,)),
            pltpu.SemaphoreType.DMA((15,)),
        ],
        compiler_params=pltpu.CompilerParams(
            vmem_limit_bytes=VMEM_LIMIT,
            dimension_semantics=("arbitrary",),
            collective_id=0,
            has_side_effects=True,
        ),
        cost_estimate=pl.CostEstimate(
            flops=8 * tokens * d * bf * blocks,
            bytes_accessed=4 * d * bf * blocks,
            transcendentals=2 * tokens * bf * blocks,
        ),
        name="gather_up",
    )(x, small, sg, su)


def up_down(x, xs, h, inits, off, sg, su, sd, bf):
    half, d = x.shape
    m, early = 2 * half, h.shape[1] // bf
    blocks = sd.shape[0] // 2 // bf
    late = blocks - early

    def kern(off_ref, xa_ref, xs_ref, ia_ref, ib_ref, g_ref, u_ref, h_ref, d_ref, *rest):
        own_ref, sib_ref, x2, hs, acc, sems = rest
        i = pl.program_id(0)
        copies = [
            pltpu.make_async_copy(src, dst, sems.at[n])
            for n, (src, dst) in enumerate(
                (
                    (xa_ref, x2.at[pl.ds(0, half)]),
                    (xs_ref.at[CORE - 1], x2.at[pl.ds(half, half)]),
                    (ia_ref, acc.at[pl.ds(0, half)]),
                    (ib_ref, acc.at[pl.ds(half, half)]),
                )
            )
        ]

        @pl.when(i == 0)
        def _():
            for c in copies:
                c.start()
            copies[0].wait()
            copies[1].wait()

        @pl.when(i < late)
        def _():
            hs[i] = swiglu(dot(x2[...], g_ref[...]), dot(x2[...], u_ref[...]))

        @pl.when(i == late)
        def _():
            copies[2].wait()
            copies[3].wait()

        @pl.when((i >= late) & (i < 2 * late))
        def _():
            acc[...] += dot(hs[i - late], d_ref[...])

        @pl.when(i >= 2 * late)
        def _():
            acc[...] += dot(h_ref[...], d_ref[...])

        @pl.when(i == late + blocks - 1)
        def _():
            own_ref[...] = acc[:half]
            sib_ref[...] = acc[half:].astype(jnp.bfloat16)

    def column(i, o):
        return (0, o[0] + early + jnp.minimum(i, late - 1))

    def row(i, o):
        j = jnp.maximum(i - late, 0)
        return (o[0] + jnp.where(j < late, early + j, j - late), 0)

    any_spec = pl.BlockSpec(memory_space=pl.ANY)
    return pl.pallas_call(
        kern,
        out_shape=[
            jax.ShapeDtypeStruct((half, d), jnp.float32),
            jax.ShapeDtypeStruct((half, d), jnp.bfloat16),
        ],
        grid_spec=pltpu.PrefetchScalarGridSpec(
            num_scalar_prefetch=1,
            grid=(late + blocks,),
            in_specs=[any_spec] * 4
            + [pl.BlockSpec((d, bf), column)] * 2
            + [
                pl.BlockSpec((m, bf), lambda i, o: (0, jnp.maximum(i - 2 * late, 0))),
                pl.BlockSpec((bf, d), row),
            ],
            out_specs=[pl.BlockSpec((half, d), lambda i, o: (0, 0))] * 2,
            scratch_shapes=[
                pltpu.VMEM((m, d), jnp.bfloat16),
                pltpu.VMEM((late, m, bf), jnp.bfloat16),
                pltpu.VMEM((m, d), jnp.float32),
                pltpu.SemaphoreType.DMA((4,)),
            ],
        ),
        compiler_params=params(1),
        cost_estimate=pl.CostEstimate(
            flops=2 * m * d * bf * (blocks + 2 * late),
            bytes_accessed=2 * d * bf * (blocks + 2 * late),
            transcendentals=m * bf * late,
        ),
        name="up_down",
    )(off, x, xs, *inits, sg, su, h, sd)


def routed_call(x, xs, codes, eoff, wg, wu, wd, experts, slots, bf):
    n_src = 1 + xs.shape[0]
    groups = n_src // 4
    d = x.shape[1]
    ff = wg.shape[2]
    nf = ff // bf
    chunks = slots // CHUNK
    top, tokens = codes.shape[1:]

    def kern(eoff_ref, code_ref, *rest):
        x_ref, xs_ref, g_ref, u_ref, d_ref, out_ref, z, acc, used = rest
        e, f = pl.program_id(0), pl.program_id(1)

        @pl.when(f == 0)
        def _():
            low = (e * slots).astype(jnp.float32)
            row = low + lax.broadcasted_iota(jnp.int32, (slots, tokens), 0).astype(jnp.float32)
            for grp in range(groups):
                most = jnp.full((top, tokens), -1.0, jnp.float32)
                for k in range(4):
                    s = grp * 4 + k
                    code = code_ref[s]
                    here = (code >= low) & (code < low + slots)
                    most = jnp.maximum(most, jnp.where(here, code - low, -1.0))
                    pick = jnp.zeros((slots, tokens), jnp.float32)
                    for j in range(top):
                        pick = jnp.where(row == code[j : j + 1, :], 1.0, pick)
                    pick = pick.astype(jnp.bfloat16)
                    zs = dot(pick, x_ref[...] if s == 0 else xs_ref[s - 1])
                    z[grp, :, k] = zs.astype(jnp.bfloat16).reshape(chunks, CHUNK, d)
                used[grp] = (jnp.max(most).astype(jnp.int32) + CHUNK) // CHUNK
            acc[...] = jnp.zeros_like(acc)

        for grp in range(groups):
            for v in range(1, chunks + 1):

                @pl.when(used[grp] == v)
                def _(grp=grp, v=v):
                    m = v * 4 * CHUNK
                    zz = z[grp, :v].reshape(m, d)
                    h = swiglu(dot(zz, g_ref[0]), dot(zz, u_ref[0]))
                    acc[grp, :m] += dot(h, d_ref[0])

        @pl.when(f == nf - 1)
        def _():
            out_ref[0] = acc[...].astype(jnp.bfloat16).reshape(groups, chunks, 4, CHUNK, d)

    rows = chunks * 4 * CHUNK
    total = experts * groups * rows
    return pl.pallas_call(
        kern,
        out_shape=jax.ShapeDtypeStruct((experts, groups, chunks, 4, CHUNK, d), jnp.bfloat16),
        grid_spec=pltpu.PrefetchScalarGridSpec(
            num_scalar_prefetch=1,
            grid=(experts, nf),
            in_specs=[pl.BlockSpec(codes.shape, lambda e, f, o: (0, 0, 0))]
            + [
                pl.BlockSpec(x.shape, lambda e, f, o: (0, 0), pipeline_mode=pl.Buffered(1)),
                pl.BlockSpec(xs.shape, lambda e, f, o: (0, 0, 0), pipeline_mode=pl.Buffered(1)),
            ]
            + [
                pl.BlockSpec((1, d, bf), lambda e, f, o: (o[0] + e, 0, f)),
                pl.BlockSpec((1, d, bf), lambda e, f, o: (o[0] + e, 0, f)),
                pl.BlockSpec((1, bf, d), lambda e, f, o: (o[0] + e, f, 0)),
            ],
            out_specs=pl.BlockSpec(
                (1, groups, chunks, 4, CHUNK, d), lambda e, f, o: (e, 0, 0, 0, 0, 0)
            ),
            scratch_shapes=[
                pltpu.VMEM((groups, chunks, 4, CHUNK, d), jnp.bfloat16),
                pltpu.VMEM((groups, rows, d), jnp.float32),
                pltpu.SMEM((groups,), jnp.int32),
            ],
        ),
        compiler_params=params(2),
        cost_estimate=pl.CostEstimate(
            flops=4 * total * d * ff,
            bytes_accessed=6 * experts * d * ff,
            transcendentals=total * ff,
        ),
        name="routed",
    )(eoff, codes, x, xs, wg, wu, wd)


def combine_call(out, codes, gates, sources, types, adds, slots, name, pieces=1):
    experts, groups, chunks, _, _, d = out.shape
    top, tokens = codes.shape[1:]
    n = len(sources)
    flat = [a for part in adds for a, _ in part]
    bn = 896

    def kern(code_ref, gate_ref, *rest):
        out_refs, add_refs = rest[:n], list(rest[n : n + len(flat)])
        y_refs, weights = rest[n + len(flat) : -1], rest[-1]

        @pl.when(pl.program_id(0) == 0)
        def _():
            row = lax.broadcasted_iota(jnp.int32, (experts * slots, tokens), 0)
            row = row.astype(jnp.float32)
            for i, s in enumerate(sources):
                weight = jnp.zeros(row.shape, jnp.float32)
                for j in range(top):
                    weight = jnp.where(
                        row == code_ref[s, j : j + 1, :], gate_ref[s, j : j + 1, :], weight
                    )
                weights[i] = weight.T.astype(jnp.bfloat16)

        def put(i, y):
            m = tokens // pieces
            for p in range(pieces):
                y_refs[i * pieces + p][...] = y[p * m : (p + 1) * m].astype(types[i])

        at = 0
        for i in range(n):
            y = dot(weights[i], out_refs[i][...].reshape(experts * slots, bn))
            if not adds or not adds[i]:
                put(i, y)
                continue
            parts = [y]
            for a, first in adds[i]:
                m, v = a.shape[0], add_refs[at][...].astype(jnp.float32)
                at += 1
                if m < tokens:
                    zero = jnp.zeros((tokens - m, bn), jnp.float32)
                    v = jnp.concatenate([v, zero] if first == 0 else [zero, v])
                parts.append(v)
            put(i, sum(parts))

    return pl.pallas_call(
        kern,
        out_shape=[
            jax.ShapeDtypeStruct((tokens // pieces, d), t) for t in types for _ in range(pieces)
        ],
        grid=(d // bn,),
        in_specs=[pl.BlockSpec(codes.shape, lambda n: (0, 0, 0))] * 2
        + [
            pl.BlockSpec(
                (experts, 1, chunks, 1, CHUNK, bn),
                lambda n, s=s: (0, s // 4, 0, s % 4, 0, n),
            )
            for s in sources
        ]
        + [pl.BlockSpec((a.shape[0], bn), lambda n: (0, n)) for a in flat],
        out_specs=[pl.BlockSpec((tokens // pieces, bn), lambda n: (0, n))] * (n * pieces),
        scratch_shapes=[pltpu.VMEM((n, tokens, experts * slots), jnp.bfloat16)],
        compiler_params=params(1),
        cost_estimate=pl.CostEstimate(
            flops=2 * n * tokens * experts * slots * d,
            bytes_accessed=2 * n * experts * slots * d,
            transcendentals=0,
        ),
        name=name,
    )(codes, gates, *([out] * n), *flat)


def solution(mesh):
    groups = mesh.shape["dp"]

    def swap(v, bit):
        return lax.ppermute(v, ("dp", "ep"), [(i, i ^ bit) for i in range(8)])

    after = lax.optimization_barrier

    def body(x, expert, slot, gate, wg, wu, wd, sg, su, sd):
        x = x[0, 0]
        tokens, d = x.shape
        half = tokens // 2
        top, ff = expert.shape[-1], sg.shape[1]
        slots = 5 * tokens * top // (4 * wg.shape[0] * mesh.shape["ep"])
        experts = wg.shape[0] // groups
        me, part = lax.axis_index("ep"), lax.axis_index("dp")
        bf = 512
        blocks = ff // 2 // bf
        early, relay = 15, 10
        off = jnp.reshape((me % 2) * blocks, (1,)).astype(jnp.int32)
        eoff = jnp.reshape(part * experts, (1,)).astype(jnp.int32)

        code = jnp.where(slot < slots, expert * slots + slot, -1)[0, 0]
        weight = gate[0, 0].astype(jnp.bfloat16).astype(jnp.float32)
        small = jnp.stack([code.astype(jnp.float32).T, weight.T])
        h, xs, smalls = gather_up(x, small, sg, su, blocks, early, relay, bf)
        smalls = jnp.concatenate([small[None], smalls])
        base = (me * wg.shape[0] + part * experts) * slots
        codes = smalls[:, 0] - base.astype(jnp.float32)
        gates = smalls[:, 1]

        out = routed_call(x, xs, codes, eoff, wg, wu, wd, experts, slots, 512)

        f32, bf16 = jnp.float32, jnp.bfloat16

        def combine(sources, types, adds, name):
            return combine_call(out, codes, gates, sources, types, adds, slots, name)

        (cxy,) = combine((7,), (bf16,), (), "combine_diag_core")
        adds = [[(swap(cxy, CORE), 0)]]
        t, b = combine_call(
            out, codes, gates, (6,), (bf16,), adds, slots, "combine_diag", pieces=2
        )
        t, b, codes_b = after((t, b, codes))
        t, b = swap(t, Y), swap(b, X)
        cx, cy = combine_call(
            out, codes_b, gates, (3, 5), (bf16,) * 2, (), slots, "combine_core"
        )
        cx, cy, codes_c = after((cx, cy, codes))
        cx, cy = swap(cx, CORE), swap(cy, CORE)
        near = combine_call(out, codes_c, gates, (0, 1), (f32,) * 2, (), slots, "combine_near")
        near, t, b, cx, cy = after((near, t, b, cx, cy))
        qx, qy = combine(
            (2, 4), (bf16,) * 2, [[(cx, 0), (t, 0)], [(cy, 0), (b, half)]], "combine_mid"
        )
        near, qx, qy = after((near, qx, qy))
        qx, qy = swap(qx, X), swap(qy, Y)
        own, sib = up_down(x, xs, h, near, off, sg, su, sd, bf)
        own, sib, qx, qy = after((own, sib, qx, qy))
        y = own + swap(sib, CORE).astype(f32) + qx.astype(f32) + qy.astype(f32)
        return y.astype(bf16)[None, None]

    lead = P("dp", "ep", None, None)
    return jax.shard_map(
        body,
        mesh=mesh,
        in_specs=(lead,) * 4 + (P("ep", None, None),) * 3 + (P(None, None),) * 3,
        out_specs=lead,
        check_vma=False,
    )
```

```python
import jax
import jax.numpy as jnp
from jax import lax
from jax.experimental import pallas as pl
from jax.experimental.pallas import tpu as pltpu
from jax.sharding import PartitionSpec as P

CHUNK = 16
VMEM_LIMIT = 66_500_000
X, Y, CORE = 2, 4, 1


def dot(a, b):
    return jnp.dot(a, b, preferred_element_type=jnp.float32)


def swiglu(g, u):
    return (g * jax.nn.sigmoid(g) * u).astype(jnp.bfloat16)


def params(n):
    return pltpu.CompilerParams(
        vmem_limit_bytes=VMEM_LIMIT, dimension_semantics=("arbitrary",) * n
    )


def place():
    ep = lax.axis_index("ep")
    return lax.axis_index("dp"), ep // 2, ep % 2


def peer(bits):
    y, x, core = place()
    y = 1 - y if bits & Y else y
    x = 1 - x if bits & X else x
    core = 1 - core if bits & CORE else core
    return (y, x * 2 + core)


def gather_up(x, small, sg, su, per_core, blocks, relay, bf):
    tokens, d = x.shape
    half = tokens // 2

    def kern(x_ref, small_ref, g_ref, u_ref, h_ref, all_x, all_small, x2, local, send, recv):
        i = pl.program_id(0)

        def copy(n, src, dst, bits):
            return pltpu.make_async_remote_copy(
                src_ref=src,
                dst_ref=dst,
                send_sem=send.at[n],
                recv_sem=recv.at[n],
                device_id=peer(bits),
                device_id_type=pl.DeviceIdType.MESH,
            )

        def at(bits):
            return all_x.at[bits - 1]

        top, bottom = pl.ds(0, half), pl.ds(half, half)
        first = [copy(n, x_ref, at(b), b) for n, b in enumerate((CORE, X, Y))]
        second = [
            copy(3, at(Y).at[top], at(X | Y).at[top], X),
            copy(4, at(X).at[bottom], at(X | Y).at[bottom], Y),
            copy(5, at(X), at(X | CORE), CORE),
            copy(6, at(Y), at(Y | CORE), CORE),
        ]
        third = [copy(7, at(X | Y), at(X | Y | CORE), CORE)]
        little = [copy(7 + b, small_ref, all_small.at[b - 1], b) for b in range(1, 8)]

        def up(v):
            return swiglu(dot(v, g_ref[...]), dot(v, u_ref[...]))

        @pl.when(i == 0)
        def _():
            own = pltpu.make_async_copy(x_ref, x2.at[pl.ds(0, tokens)], local.at[0])
            own.start()
            barrier = pltpu.get_barrier_semaphore()
            for bits in range(1, 8):
                pl.semaphore_signal(
                    barrier, inc=1, device_id=peer(bits), device_id_type=pl.DeviceIdType.MESH
                )
            pl.semaphore_wait(barrier, 7)
            for c in little + first:
                c.start()
            own.wait()
            h_ref[:tokens] = up(x2[:tokens])
            first[0].wait_recv()
            other = pltpu.make_async_copy(at(CORE), x2.at[pl.ds(tokens, tokens)], local.at[1])
            other.start()
            other.wait()
            h_ref[tokens:] = up(x2[tokens:])

        @pl.when(i == relay)
        def _():
            first[1].wait_recv()
            first[2].wait_recv()
            for c in second:
                c.start()

        @pl.when(i > 0)
        def _():
            h_ref[...] = up(x2[...])

        @pl.when(i == blocks - 1)
        def _():
            second[0].wait_recv()
            second[1].wait_recv()
            third[0].start()
            second[2].wait_recv()
            second[3].wait_recv()
            for c in little:
                c.wait_recv()
            third[0].wait_recv()
            for c in first + second + third + little:
                c.wait_send()

    def column(i):
        return (0, (lax.axis_index("ep") % 2) * per_core + i)

    any_spec = pl.BlockSpec(memory_space=pl.ANY)
    return pl.pallas_call(
        kern,
        out_shape=[
            jax.ShapeDtypeStruct((2 * tokens, blocks * bf), jnp.bfloat16),
            jax.ShapeDtypeStruct((7, tokens, d), x.dtype),
            jax.ShapeDtypeStruct((7, *small.shape), small.dtype),
        ],
        grid=(blocks,),
        in_specs=[any_spec] * 2 + [pl.BlockSpec((d, bf), column)] * 2,
        out_specs=[pl.BlockSpec((2 * tokens, bf), lambda i: (0, i)), any_spec, any_spec],
        scratch_shapes=[
            pltpu.VMEM((2 * tokens, d), jnp.bfloat16),
            pltpu.SemaphoreType.DMA((2,)),
            pltpu.SemaphoreType.DMA((15,)),
            pltpu.SemaphoreType.DMA((15,)),
        ],
        compiler_params=pltpu.CompilerParams(
            vmem_limit_bytes=VMEM_LIMIT,
            dimension_semantics=("arbitrary",),
            collective_id=0,
            has_side_effects=True,
        ),
        cost_estimate=pl.CostEstimate(
            flops=8 * tokens * d * bf * blocks,
            bytes_accessed=4 * d * bf * blocks,
            transcendentals=2 * tokens * bf * blocks,
        ),
        name="gather_up",
    )(x, small, sg, su)


def reduce_up_down(x, xs, h, out, codes, gates, sg, su, sd, slots, bf):
    half, d = x.shape
    mid = half // 2
    experts, _, chunks = out.shape[:3]
    rows = experts * slots
    top = codes.shape[1]
    m, early = 2 * half, h.shape[1] // bf
    blocks = sd.shape[0] // 2 // bf
    late = blocks - early
    bu = bf // 2
    ups = 2 * late
    order = (7, 5, 3, 6, 1, 0)
    up0 = len(order)
    mid0 = up0 + ups
    down0 = mid0 + 2
    steps = down0 + blocks
    bn = 512
    f32, bf16 = jnp.float32, jnp.bfloat16

    def kern(*refs):
        code_ref, gate_ref, x_ref, xs_ref, out_ref, g_ref, u_ref, h_ref, d_ref, y_ref = refs[:10]
        x2, hs, acc, weight, sends, cores, links, t_ref, b_ref, local, send, recv = refs[10:]
        i = pl.program_id(0)
        top_half, bottom = pl.ds(0, mid), pl.ds(mid, mid)
        own, other = pl.ds(0, half), pl.ds(half, half)
        moves = [
            (sends.at[0], cores.at[0], CORE),
            (sends.at[1], cores.at[1], CORE),
            (x2.at[other], cores.at[2], CORE),
            (sends.at[0].at[top_half], t_ref, Y),
            (sends.at[0].at[bottom], b_ref, X),
            (x2.at[own], links.at[0], X),
            (x2.at[other], links.at[1], Y),
            (sends.at[0], cores.at[3], CORE),
        ]
        copies = [
            pltpu.make_async_remote_copy(
                src_ref=src,
                dst_ref=dst,
                send_sem=send.at[n],
                recv_sem=recv.at[n],
                device_id=peer(bits),
                device_id_type=pl.DeviceIdType.MESH,
            )
            for n, (src, dst, bits) in enumerate(moves)
        ]
        loads = [
            pltpu.make_async_copy(x_ref, x2.at[own], local.at[0]),
            pltpu.make_async_copy(xs_ref.at[CORE - 1], x2.at[other], local.at[1]),
        ]

        def combine(s, put):
            row = lax.broadcasted_iota(jnp.int32, (rows, half), 0).astype(f32)
            w = jnp.zeros(row.shape, f32)
            for j in range(top):
                w = jnp.where(row == code_ref[s, j : j + 1, :], gate_ref[s, j : j + 1, :], w)
            weight[...] = w.T.astype(bf16)

            @pl.loop(0, d // bn)
            def _(n):
                cols = pl.ds(pl.multiple_of(n * bn, bn), bn)
                put(cols, dot(weight[...], out_ref[:, 0, :, 0, :, cols].reshape(rows, bn)))

        @pl.when(i == 0)
        def _():
            barrier = pltpu.get_barrier_semaphore()
            for bits in (CORE, X, Y):
                pl.semaphore_signal(
                    barrier, inc=1, device_id=peer(bits), device_id_type=pl.DeviceIdType.MESH
                )

        for n in range(3):

            @pl.when(i == n)
            def _(n=n):
                def put(cols, y):
                    if n < 2:
                        sends[n, :, cols] = y.astype(bf16)
                    else:
                        x2[other, cols] = y.astype(bf16)

                combine(order[n], put)
                if n == 0:
                    pl.semaphore_wait(pltpu.get_barrier_semaphore(), 3)
                copies[n].start()

        @pl.when(i == 3)
        def _():
            copies[0].wait_send()
            copies[0].wait_recv()

            def put(cols, y):
                sends[0, :, cols] = (y + cores[0, :, cols].astype(f32)).astype(bf16)

            combine(order[3], put)
            copies[3].start()
            copies[4].start()

        for n, where in ((4, other), (5, own)):

            @pl.when(i == n)
            def _(n=n, where=where):
                def put(cols, y):
                    acc[where, cols] = y

                if n == 5:
                    copies[2].wait_send()
                    for c in loads:
                        c.start()
                combine(order[n], put)
                if n == 5:
                    for c in loads:
                        c.wait()

        @pl.when((i >= up0) & (i < mid0))
        def _():
            hs[i - up0] = swiglu(dot(x2[...], g_ref[...]), dot(x2[...], u_ref[...]))

        @pl.when(i == mid0)
        def _():
            copies[2].wait_recv()
            copies[3].wait_recv()

            def put(cols, y):
                y = y + cores[2, :, cols].astype(f32)
                x2[top_half, cols] = (y[:mid] + t_ref[:, cols].astype(f32)).astype(bf16)
                x2[bottom, cols] = y[mid:].astype(bf16)

            combine(2, put)
            copies[5].start()

        @pl.when(i == mid0 + 1)
        def _():
            copies[1].wait_send()
            copies[1].wait_recv()
            copies[4].wait_recv()

            def put(cols, y):
                y = y + cores[1, :, cols].astype(f32)
                x2[pl.ds(half, mid), cols] = y[:mid].astype(bf16)
                x2[pl.ds(half + mid, mid), cols] = (
                    y[mid:] + b_ref[:, cols].astype(f32)
                ).astype(bf16)

            combine(4, put)
            copies[6].start()

        @pl.when((i >= down0) & (i < down0 + late))
        def _():
            j = 2 * (i - down0)
            acc[...] += dot(hs[j], d_ref[:bu]) + dot(hs[j + 1], d_ref[bu:])

        @pl.when(i >= down0 + late)
        def _():
            acc[...] += dot(h_ref[...], d_ref[...])

        @pl.when(i == steps - 1)
        def _():
            copies[3].wait_send()
            copies[4].wait_send()
            sends[0] = acc[other].astype(bf16)
            copies[7].start()
            copies[5].wait_recv()
            copies[6].wait_recv()
            acc[own] += links[0].astype(f32) + links[1].astype(f32)
            copies[7].wait_recv()
            sends[1] = (acc[own] + cores[3].astype(f32)).astype(bf16)
            result = pltpu.make_async_copy(sends.at[1], y_ref, local.at[0])
            result.start()
            for n in (5, 6, 7):
                copies[n].wait_send()
            result.wait()

    def core():
        return lax.axis_index("ep") % 2

    def source(i):
        s = jnp.where(i <= mid0, 2, 4)
        for n, v in enumerate(order):
            s = jnp.where(i == n, v, s)
        return (0, s // 4, 0, s % 4, 0, 0)

    def column(i):
        return (0, 2 * (core() * blocks + early) + jnp.clip(i - up0, 0, ups - 1))

    def down_row(i):
        j = jnp.maximum(i - down0, 0)
        return (core() * blocks + jnp.where(j < late, early + j, j - late), 0)

    any_spec = pl.BlockSpec(memory_space=pl.ANY)
    small_spec = pl.BlockSpec(codes.shape, lambda i: (0, 0, 0))
    dma = pltpu.SemaphoreType.DMA
    return pl.pallas_call(
        kern,
        out_shape=jax.ShapeDtypeStruct((half, d), bf16),
        grid=(steps,),
        in_specs=[small_spec, small_spec, any_spec, any_spec]
        + [pl.BlockSpec((experts, 1, chunks, 1, CHUNK, d), source)]
        + [pl.BlockSpec((d, bu), column)] * 2
        + [
            pl.BlockSpec((m, bf), lambda i: (0, jnp.maximum(i - down0 - late, 0))),
            pl.BlockSpec((bf, d), down_row),
        ],
        out_specs=any_spec,
        scratch_shapes=[
            pltpu.VMEM((m, d), bf16),
            pltpu.VMEM((ups, m, bu), bf16),
            pltpu.VMEM((m, d), f32),
            pltpu.VMEM((half, rows), bf16),
            pltpu.VMEM((2, half, d), bf16),
            pltpu.VMEM((4, half, d), bf16),
            pltpu.VMEM((2, half, d), bf16),
            pltpu.VMEM((mid, d), bf16),
            pltpu.VMEM((mid, d), bf16),
            dma((2,)),
            dma((8,)),
            dma((8,)),
        ],
        compiler_params=pltpu.CompilerParams(
            vmem_limit_bytes=VMEM_LIMIT,
            dimension_semantics=("arbitrary",),
            collective_id=1,
            has_side_effects=True,
        ),
        cost_estimate=pl.CostEstimate(
            flops=2 * m * d * bf * (blocks + 2 * late),
            bytes_accessed=2 * d * bf * (blocks + 2 * late),
            transcendentals=m * bf * late,
        ),
        name="reduce_up_down",
    )(codes, gates, x, xs, out, sg, su, h, sd)


def plan_call(smalls, base, part, slots):
    n_src, _, top, tokens = smalls.shape
    groups = n_src // 4
    experts = 4 * groups

    def kern(base_ref, part_ref, small_ref, code_ref, expert_ref, used_ref):
        low = base_ref[0].astype(jnp.float32)
        codes = [small_ref[s, 0] - low for s in range(n_src)]
        used, total = [], []
        for e in range(experts):
            counts = []
            for grp in range(groups):
                most = jnp.full((top, tokens), -1.0, jnp.float32)
                for s in range(grp * 4, grp * 4 + 4):
                    here = (codes[s] >= e * slots) & (codes[s] < (e + 1) * slots)
                    most = jnp.maximum(most, jnp.where(here, codes[s] - e * slots, -1.0))
                counts.append((jnp.max(most).astype(jnp.int32) + CHUNK) // CHUNK)
            used.append(counts)
            total.append(sum(counts))
        news = [jnp.full((top, tokens), -1.0, jnp.float32) for _ in range(n_src)]
        for e in range(experts):
            rank = jnp.int32(0)
            for o in range(experts):
                if o != e:
                    ahead = total[o] >= total[e] if o < e else total[o] > total[e]
                    rank = rank + ahead.astype(jnp.int32)
            spot = rank // 2
            mine = (rank % 2 + spot % 2) % 2 == part_ref[0]

            @pl.when(mine)
            def _(e=e, spot=spot):
                expert_ref[spot] = e
                for grp in range(groups):
                    used_ref[spot, grp] = used[e][grp]

            shift = jnp.where(mine, (spot - e) * slots, -(10**6)).astype(jnp.float32)
            for s in range(n_src):
                here = (codes[s] >= e * slots) & (codes[s] < (e + 1) * slots)
                news[s] = jnp.where(here, codes[s] + shift, news[s])
        for s in range(n_src):
            code_ref[s] = news[s]

    smem = pl.BlockSpec(memory_space=pltpu.SMEM)
    return pl.pallas_call(
        kern,
        out_shape=[
            jax.ShapeDtypeStruct((n_src, top, tokens), jnp.float32),
            jax.ShapeDtypeStruct((experts // groups,), jnp.int32),
            jax.ShapeDtypeStruct((experts // groups, groups), jnp.int32),
        ],
        in_specs=[smem, smem, pl.BlockSpec(memory_space=pltpu.VMEM)],
        out_specs=[pl.BlockSpec(memory_space=pltpu.VMEM), smem, smem],
        name="plan",
    )(base, part, smalls)


def routed_call(x, xs, codes, picked, used, wg, wu, wd, slots, bf):
    n_src = 1 + xs.shape[0]
    groups = n_src // 4
    experts = picked.shape[0]
    d = x.shape[1]
    ff = wg.shape[2]
    nf = ff // bf
    chunks = slots // CHUNK
    top, tokens = codes.shape[1:]
    rows = 4 * CHUNK
    whole = 6

    def kern(picked_ref, used_ref, code_ref, x_ref, xs_ref, g_ref, u_ref, d_ref, out_ref, z, acc):
        e, f = pl.program_id(0), pl.program_id(1)
        lead = used_ref[e, 0]
        total = lead + used_ref[e, 1]

        @pl.when((e == 0) & (f == 0))
        def _():
            acc[...] = jnp.zeros_like(acc)

        @pl.when(f == 0)
        def _():
            low = (e * slots).astype(jnp.float32)
            row = low + lax.broadcasted_iota(jnp.int32, (slots, tokens), 0).astype(jnp.float32)
            for grp in range(groups):
                for k in range(4):
                    s = grp * 4 + k
                    pick = jnp.zeros((slots, tokens), jnp.float32)
                    for j in range(top):
                        pick = jnp.where(row == code_ref[s, j : j + 1, :], 1.0, pick)
                    pick = pick.astype(jnp.bfloat16)
                    zs = dot(pick, x_ref[...] if s == 0 else xs_ref[s - 1])
                    zs = zs.astype(jnp.bfloat16).reshape(chunks, CHUNK, d)
                    z[pl.ds(0 if grp == 0 else lead, chunks), k] = zs

        def part(first, n):
            m = n * rows
            zz = z[pl.ds(first, n)].reshape(m, d)
            h = swiglu(dot(zz, g_ref[0]), dot(zz, u_ref[0]))
            old = jnp.where(f == 0, 0.0, acc[pl.ds(first, n)].reshape(m, d))
            acc[pl.ds(first, n)] = (old + dot(h, d_ref[0])).reshape(n, rows, d)

        two = total > whole
        head = jnp.where(two, (total + 1) // 2, total)

        def step(i, _):
            n = jnp.where(i == 0, head, total - head)
            for v in range(1, whole + 1):
                pl.when(n == v)(lambda v=v: part(i * head, v))
            return 0

        lax.fori_loop(0, jnp.where(two, 2, 1), step, 0)

        @pl.when(f == nf - 1)
        def _():
            for grp in range(groups):
                o = acc[pl.ds(0 if grp == 0 else lead, chunks)]
                out_ref[0, grp] = o.astype(jnp.bfloat16).reshape(chunks, 4, CHUNK, d)

    total = experts * groups * chunks * rows
    return pl.pallas_call(
        kern,
        out_shape=jax.ShapeDtypeStruct((experts, groups, chunks, 4, CHUNK, d), jnp.bfloat16),
        grid_spec=pltpu.PrefetchScalarGridSpec(
            num_scalar_prefetch=2,
            grid=(experts, nf),
            in_specs=[
                pl.BlockSpec(codes.shape, lambda e, f, p, u: (0, 0, 0)),
                pl.BlockSpec(x.shape, lambda e, f, p, u: (0, 0), pipeline_mode=pl.Buffered(1)),
                pl.BlockSpec(
                    xs.shape, lambda e, f, p, u: (0, 0, 0), pipeline_mode=pl.Buffered(1)
                ),
                pl.BlockSpec((1, d, bf), lambda e, f, p, u: (p[e], 0, f)),
                pl.BlockSpec((1, d, bf), lambda e, f, p, u: (p[e], 0, f)),
                pl.BlockSpec((1, bf, d), lambda e, f, p, u: (p[e], f, 0)),
            ],
            out_specs=pl.BlockSpec(
                (1, groups, chunks, 4, CHUNK, d), lambda e, f, p, u: (e, 0, 0, 0, 0, 0)
            ),
            scratch_shapes=[
                pltpu.VMEM((groups * chunks, 4, CHUNK, d), jnp.bfloat16),
                pltpu.VMEM((groups * chunks, rows, d), jnp.float32),
            ],
        ),
        compiler_params=params(2),
        cost_estimate=pl.CostEstimate(
            flops=4 * total * d * ff,
            bytes_accessed=6 * experts * d * ff,
            transcendentals=total * ff,
        ),
        name="routed",
    )(picked, used, codes, x, xs, wg, wu, wd)


def solution(mesh):
    def body(x, expert, slot, gate, wg, wu, wd, sg, su, sd):
        x = x[0, 0]
        tokens = x.shape[0]
        top, ff = expert.shape[-1], sg.shape[1]
        slots = 5 * tokens * top // (4 * wg.shape[0] * mesh.shape["ep"])
        me, part = lax.axis_index("ep"), lax.axis_index("dp")
        bf = 512
        blocks = ff // 2 // bf
        early, relay = 15, 10

        code = jnp.where(slot < slots, expert * slots + slot, -1)[0, 0]
        weight = gate[0, 0].astype(jnp.bfloat16).astype(jnp.float32)
        small = jnp.stack([code.astype(jnp.float32).T, weight.T])
        h, xs, smalls = gather_up(x, small, sg, su, blocks, early, relay, bf)
        smalls = jnp.concatenate([small[None], smalls])
        base = jnp.reshape(me * wg.shape[0] * slots, (1,)).astype(jnp.int32)
        mine = jnp.reshape(part, (1,)).astype(jnp.int32)
        codes, picked, used = plan_call(smalls, base, mine, slots)
        gates = smalls[:, 1]
        out = routed_call(x, xs, codes, picked, used, wg, wu, wd, slots, 512)

        y = reduce_up_down(x, xs, h, out, codes, gates, sg, su, sd, slots, bf)
        return y[None, None]

    lead = P("dp", "ep", None, None)
    return jax.shard_map(
        body,
        mesh=mesh,
        in_specs=(lead,) * 4 + (P("ep", None, None),) * 3 + (P(None, None),) * 3,
        out_specs=lead,
        check_vma=False,
    )
```

```python
import jax
import jax.numpy as jnp
from jax import lax
from jax.experimental import pallas as pl
from jax.experimental.pallas import tpu as pltpu
from jax.sharding import PartitionSpec as P

CHUNK = 16
VMEM_LIMIT = 66_500_000
X, Y, CORE = 2, 4, 1


def dot(a, b):
    return jnp.dot(a, b, preferred_element_type=jnp.float32)


def swiglu(g, u):
    return (g * jax.nn.sigmoid(g) * u).astype(jnp.bfloat16)


def params(n):
    return pltpu.CompilerParams(
        vmem_limit_bytes=VMEM_LIMIT, dimension_semantics=("arbitrary",) * n
    )


def place():
    ep = lax.axis_index("ep")
    return lax.axis_index("dp"), ep // 2, ep % 2


def peer(bits):
    y, x, core = place()
    y = 1 - y if bits & Y else y
    x = 1 - x if bits & X else x
    core = 1 - core if bits & CORE else core
    return (y, x * 2 + core)


def gather_up(x, small, sg, su, per_core, blocks, relay, bf):
    tokens, d = x.shape
    half = tokens // 2

    def kern(x_ref, small_ref, g_ref, u_ref, h_ref, all_x, all_small, x2, local, send, recv):
        i = pl.program_id(0)

        def copy(n, src, dst, bits):
            return pltpu.make_async_remote_copy(
                src_ref=src,
                dst_ref=dst,
                send_sem=send.at[n],
                recv_sem=recv.at[n],
                device_id=peer(bits),
                device_id_type=pl.DeviceIdType.MESH,
            )

        def at(bits):
            return all_x.at[bits - 1]

        top, bottom = pl.ds(0, half), pl.ds(half, half)
        first = [copy(n, x_ref, at(b), b) for n, b in enumerate((CORE, X, Y))]
        second = [
            copy(3, at(Y).at[top], at(X | Y).at[top], X),
            copy(4, at(X).at[bottom], at(X | Y).at[bottom], Y),
            copy(5, at(X), at(X | CORE), CORE),
            copy(6, at(Y), at(Y | CORE), CORE),
        ]
        third = [copy(7, at(X | Y), at(X | Y | CORE), CORE)]
        little = [copy(7 + b, small_ref, all_small.at[b - 1], b) for b in range(1, 8)]

        def up(v):
            return swiglu(dot(v, g_ref[...]), dot(v, u_ref[...]))

        @pl.when(i == 0)
        def _():
            own = pltpu.make_async_copy(x_ref, x2.at[pl.ds(0, tokens)], local.at[0])
            own.start()
            barrier = pltpu.get_barrier_semaphore()
            for bits in range(1, 8):
                pl.semaphore_signal(
                    barrier, inc=1, device_id=peer(bits), device_id_type=pl.DeviceIdType.MESH
                )
            pl.semaphore_wait(barrier, 7)
            for c in little + first:
                c.start()
            own.wait()
            h_ref[:tokens] = up(x2[:tokens])
            first[0].wait_recv()
            other = pltpu.make_async_copy(at(CORE), x2.at[pl.ds(tokens, tokens)], local.at[1])
            other.start()
            other.wait()
            h_ref[tokens:] = up(x2[tokens:])

        @pl.when(i == relay)
        def _():
            first[1].wait_recv()
            first[2].wait_recv()
            for c in second:
                c.start()

        @pl.when(i == blocks - 1)
        def _():
            second[0].wait_recv()
            second[1].wait_recv()
            third[0].start()

        @pl.when(i > 0)
        def _():
            h_ref[...] = up(x2[...])

        @pl.when(i == blocks - 1)
        def _():
            second[2].wait_recv()
            second[3].wait_recv()
            for c in little:
                c.wait_recv()
            third[0].wait_recv()
            for c in first + second + third + little:
                c.wait_send()

    def column(i):
        return (0, (lax.axis_index("ep") % 2) * per_core + i)

    any_spec = pl.BlockSpec(memory_space=pl.ANY)
    return pl.pallas_call(
        kern,
        out_shape=[
            jax.ShapeDtypeStruct((2 * tokens, blocks * bf), jnp.bfloat16),
            jax.ShapeDtypeStruct((7, tokens, d), x.dtype),
            jax.ShapeDtypeStruct((7, *small.shape), small.dtype),
        ],
        grid=(blocks,),
        in_specs=[any_spec] * 2 + [pl.BlockSpec((d, bf), column)] * 2,
        out_specs=[pl.BlockSpec((2 * tokens, bf), lambda i: (0, i)), any_spec, any_spec],
        scratch_shapes=[
            pltpu.VMEM((2 * tokens, d), jnp.bfloat16),
            pltpu.SemaphoreType.DMA((2,)),
            pltpu.SemaphoreType.DMA((15,)),
            pltpu.SemaphoreType.DMA((15,)),
        ],
        compiler_params=pltpu.CompilerParams(
            vmem_limit_bytes=VMEM_LIMIT,
            dimension_semantics=("arbitrary",),
            collective_id=0,
            has_side_effects=True,
        ),
        cost_estimate=pl.CostEstimate(
            flops=8 * tokens * d * bf * blocks,
            bytes_accessed=4 * d * bf * blocks,
            transcendentals=2 * tokens * bf * blocks,
        ),
        name="gather_up",
    )(x, small, sg, su)


def reduce_up_down(x, xs, h, out, codes, gates, sg, su, sd, slots, bf):
    half, d = x.shape
    mid = half // 2
    experts, _, chunks = out.shape[:3]
    rows = experts * slots
    top = codes.shape[1]
    m, early = 2 * half, h.shape[1] // bf
    blocks = sd.shape[0] // 2 // bf
    late = blocks - early
    bu = bf // 2
    ups = 2 * late
    order = (7, 5, 3, 6, 1, 0)
    up0 = len(order)
    mid0 = up0 + ups
    down0 = mid0 + 2
    steps = down0 + blocks
    bn = 1792
    f32, bf16 = jnp.float32, jnp.bfloat16

    def kern(*refs):
        code_ref, gate_ref, x_ref, xs_ref, out_ref, g_ref, u_ref, h_ref, d_ref, y_ref = refs[:10]
        x2, hs, acc, weight, sends, cores, links, t_ref, b_ref, local, send, recv = refs[10:]
        i = pl.program_id(0)
        top_half, bottom = pl.ds(0, mid), pl.ds(mid, mid)
        own, other = pl.ds(0, half), pl.ds(half, half)
        moves = [
            (sends.at[0], cores.at[0], CORE),
            (sends.at[1], cores.at[1], CORE),
            (x2.at[other], cores.at[2], CORE),
            (sends.at[0].at[top_half], t_ref, Y),
            (sends.at[0].at[bottom], b_ref, X),
            (x2.at[own], links.at[0], X),
            (x2.at[other], links.at[1], Y),
            (sends.at[0], cores.at[3], CORE),
        ]
        copies = [
            pltpu.make_async_remote_copy(
                src_ref=src,
                dst_ref=dst,
                send_sem=send.at[n],
                recv_sem=recv.at[n],
                device_id=peer(bits),
                device_id_type=pl.DeviceIdType.MESH,
            )
            for n, (src, dst, bits) in enumerate(moves)
        ]
        loads = [
            pltpu.make_async_copy(x_ref, x2.at[own], local.at[0]),
            pltpu.make_async_copy(xs_ref.at[CORE - 1], x2.at[other], local.at[1]),
        ]

        def combine(s, put):
            row = lax.broadcasted_iota(jnp.int32, (rows, half), 0).astype(f32)
            w = jnp.zeros(row.shape, f32)
            for j in range(top):
                w = jnp.where(row == code_ref[s, j : j + 1, :], gate_ref[s, j : j + 1, :], w)
            weight[...] = w.T.astype(bf16)

            @pl.loop(0, d // bn)
            def _(n):
                cols = pl.ds(pl.multiple_of(n * bn, bn), bn)
                put(cols, dot(weight[...], out_ref[:, 0, :, 0, :, cols].reshape(rows, bn)))

        @pl.when(i == 0)
        def _():
            barrier = pltpu.get_barrier_semaphore()
            for bits in (CORE, X, Y):
                pl.semaphore_signal(
                    barrier, inc=1, device_id=peer(bits), device_id_type=pl.DeviceIdType.MESH
                )

        for n in range(3):

            @pl.when(i == n)
            def _(n=n):
                def put(cols, y):
                    if n < 2:
                        sends[n, :, cols] = y.astype(bf16)
                    else:
                        x2[other, cols] = y.astype(bf16)

                combine(order[n], put)
                if n == 0:
                    pl.semaphore_wait(pltpu.get_barrier_semaphore(), 3)
                copies[n].start()

        @pl.when(i == 3)
        def _():
            copies[0].wait_send()
            copies[0].wait_recv()

            def put(cols, y):
                sends[0, :, cols] = (y + cores[0, :, cols].astype(f32)).astype(bf16)

            combine(order[3], put)
            copies[3].start()
            copies[4].start()

        for n, where in ((4, other), (5, own)):

            @pl.when(i == n)
            def _(n=n, where=where):
                def put(cols, y):
                    acc[where, cols] = y

                if n == 5:
                    copies[2].wait_send()
                    for c in loads:
                        c.start()
                combine(order[n], put)
                if n == 5:
                    for c in loads:
                        c.wait()

        @pl.when((i >= up0) & (i < mid0))
        def _():
            hs[i - up0] = swiglu(dot(x2[...], g_ref[...]), dot(x2[...], u_ref[...]))

        @pl.when(i == mid0)
        def _():
            copies[2].wait_recv()
            copies[3].wait_recv()

            def put(cols, y):
                y = y + cores[2, :, cols].astype(f32)
                x2[top_half, cols] = (y[:mid] + t_ref[:, cols].astype(f32)).astype(bf16)
                x2[bottom, cols] = y[mid:].astype(bf16)

            combine(2, put)
            copies[5].start()

        @pl.when(i == mid0 + 1)
        def _():
            copies[1].wait_send()
            copies[1].wait_recv()
            copies[4].wait_recv()

            def put(cols, y):
                y = y + cores[1, :, cols].astype(f32)
                x2[pl.ds(half, mid), cols] = y[:mid].astype(bf16)
                x2[pl.ds(half + mid, mid), cols] = (
                    y[mid:] + b_ref[:, cols].astype(f32)
                ).astype(bf16)

            combine(4, put)
            copies[6].start()

        @pl.when((i >= down0) & (i < down0 + late))
        def _():
            j = 2 * (i - down0)
            acc[...] += dot(hs[j], d_ref[:bu]) + dot(hs[j + 1], d_ref[bu:])

        @pl.when(i >= down0 + late)
        def _():
            acc[...] += dot(h_ref[...], d_ref[...])

        @pl.when(i == steps - 1)
        def _():
            copies[3].wait_send()
            copies[4].wait_send()
            sends[0] = acc[other].astype(bf16)
            copies[7].start()
            copies[5].wait_recv()
            copies[6].wait_recv()
            acc[own] += links[0].astype(f32) + links[1].astype(f32)
            copies[7].wait_recv()
            sends[1] = (acc[own] + cores[3].astype(f32)).astype(bf16)
            result = pltpu.make_async_copy(sends.at[1], y_ref, local.at[0])
            result.start()
            for n in (5, 6, 7):
                copies[n].wait_send()
            result.wait()

    def core():
        return lax.axis_index("ep") % 2

    def source(i):
        s = jnp.where(i <= mid0, 2, 4)
        for n, v in enumerate(order):
            s = jnp.where(i == n, v, s)
        return (0, s // 4, 0, s % 4, 0, 0)

    def column(i):
        return (0, 2 * (core() * blocks + early) + jnp.clip(i - up0, 0, ups - 1))

    def down_row(i):
        j = jnp.maximum(i - down0, 0)
        return (core() * blocks + jnp.where(j < late, early + j, j - late), 0)

    any_spec = pl.BlockSpec(memory_space=pl.ANY)
    small_spec = pl.BlockSpec(codes.shape, lambda i: (0, 0, 0))
    dma = pltpu.SemaphoreType.DMA
    return pl.pallas_call(
        kern,
        out_shape=jax.ShapeDtypeStruct((half, d), bf16),
        grid=(steps,),
        in_specs=[small_spec, small_spec, any_spec, any_spec]
        + [pl.BlockSpec((experts, 1, chunks, 1, CHUNK, d), source)]
        + [pl.BlockSpec((d, bu), column)] * 2
        + [
            pl.BlockSpec((m, bf), lambda i: (0, jnp.maximum(i - down0 - late, 0))),
            pl.BlockSpec((bf, d), down_row),
        ],
        out_specs=any_spec,
        scratch_shapes=[
            pltpu.VMEM((m, d), bf16),
            pltpu.VMEM((ups, m, bu), bf16),
            pltpu.VMEM((m, d), f32),
            pltpu.VMEM((half, rows), bf16),
            pltpu.VMEM((2, half, d), bf16),
            pltpu.VMEM((4, half, d), bf16),
            pltpu.VMEM((2, half, d), bf16),
            pltpu.VMEM((mid, d), bf16),
            pltpu.VMEM((mid, d), bf16),
            dma((2,)),
            dma((8,)),
            dma((8,)),
        ],
        compiler_params=pltpu.CompilerParams(
            vmem_limit_bytes=VMEM_LIMIT,
            dimension_semantics=("arbitrary",),
            collective_id=1,
            has_side_effects=True,
        ),
        cost_estimate=pl.CostEstimate(
            flops=2 * m * d * bf * (blocks + 2 * late),
            bytes_accessed=2 * d * bf * (blocks + 2 * late),
            transcendentals=m * bf * late,
        ),
        name="reduce_up_down",
    )(codes, gates, x, xs, out, sg, su, h, sd)


def plan_call(small, smalls, base, part, slots):
    n_src, top, tokens = 1 + smalls.shape[0], *smalls.shape[2:]
    groups = n_src // 4
    experts = 4 * groups

    def kern(base_ref, part_ref, own_ref, small_ref, code_ref, gate_ref, expert_ref, used_ref):
        low = base_ref[0].astype(jnp.float32)
        codes = [own_ref[0] - low] + [small_ref[s, 0] - low for s in range(n_src - 1)]
        gate_ref[0] = own_ref[1]
        for s in range(1, n_src):
            gate_ref[s] = small_ref[s - 1, 1]
        used, total = [], []
        for e in range(experts):
            counts = []
            for grp in range(groups):
                most = jnp.full((top, tokens), -1.0, jnp.float32)
                for s in range(grp * 4, grp * 4 + 4):
                    here = (codes[s] >= e * slots) & (codes[s] < (e + 1) * slots)
                    most = jnp.maximum(most, jnp.where(here, codes[s] - e * slots, -1.0))
                counts.append((jnp.max(most).astype(jnp.int32) + CHUNK) // CHUNK)
            used.append(counts)
            total.append(sum(counts))
        news = [jnp.full((top, tokens), -1.0, jnp.float32) for _ in range(n_src)]
        for e in range(experts):
            rank = jnp.int32(0)
            for o in range(experts):
                if o != e:
                    ahead = total[o] >= total[e] if o < e else total[o] > total[e]
                    rank = rank + ahead.astype(jnp.int32)
            spot = rank // 2
            mine = (rank % 2 + spot % 2) % 2 == part_ref[0]

            @pl.when(mine)
            def _(e=e, spot=spot):
                expert_ref[spot] = e
                for grp in range(groups):
                    used_ref[spot, grp] = used[e][grp]

            shift = jnp.where(mine, (spot - e) * slots, -(10**6)).astype(jnp.float32)
            for s in range(n_src):
                here = (codes[s] >= e * slots) & (codes[s] < (e + 1) * slots)
                news[s] = jnp.where(here, codes[s] + shift, news[s])
        for s in range(n_src):
            code_ref[s] = news[s]

    smem = pl.BlockSpec(memory_space=pltpu.SMEM)
    vmem = pl.BlockSpec(memory_space=pltpu.VMEM)
    return pl.pallas_call(
        kern,
        out_shape=[jax.ShapeDtypeStruct((n_src, top, tokens), jnp.float32)] * 2
        + [
            jax.ShapeDtypeStruct((experts // groups,), jnp.int32),
            jax.ShapeDtypeStruct((experts // groups, groups), jnp.int32),
        ],
        in_specs=[smem, smem, vmem, vmem],
        out_specs=[vmem, vmem, smem, smem],
        name="plan",
    )(base, part, small, smalls)


def routed_call(x, xs, codes, picked, used, wg, wu, wd, slots, bf):
    n_src = 1 + xs.shape[0]
    groups = n_src // 4
    experts = picked.shape[0]
    d = x.shape[1]
    ff = wg.shape[2]
    nf = ff // bf
    chunks = slots // CHUNK
    top, tokens = codes.shape[1:]
    rows = 4 * CHUNK
    whole = 6

    def kern(picked_ref, used_ref, code_ref, x_ref, xs_ref, g_ref, u_ref, d_ref, out_ref, z, acc):
        e, f = pl.program_id(0), pl.program_id(1)
        lead = used_ref[e, 0]
        total = lead + used_ref[e, 1]

        @pl.when((e == 0) & (f == 0))
        def _():
            acc[...] = jnp.zeros_like(acc)

        @pl.when(f == 0)
        def _():
            low = (e * slots).astype(jnp.float32)
            row = low + lax.broadcasted_iota(jnp.int32, (slots, tokens), 0).astype(jnp.float32)
            for grp in range(groups):
                for k in range(4):
                    s = grp * 4 + k
                    pick = jnp.zeros((slots, tokens), jnp.float32)
                    for j in range(top):
                        pick = jnp.where(row == code_ref[s, j : j + 1, :], 1.0, pick)
                    pick = pick.astype(jnp.bfloat16)
                    zs = dot(pick, x_ref[...] if s == 0 else xs_ref[s - 1])
                    zs = zs.astype(jnp.bfloat16).reshape(chunks, CHUNK, d)
                    z[pl.ds(0 if grp == 0 else lead, chunks), k] = zs

        def part(first, n):
            m = n * rows
            zz = z[pl.ds(first, n)].reshape(m, d)
            h = swiglu(dot(zz, g_ref[0]), dot(zz, u_ref[0]))
            old = jnp.where(f == 0, 0.0, acc[pl.ds(first, n)].reshape(m, d))
            acc[pl.ds(first, n)] = (old + dot(h, d_ref[0])).reshape(n, rows, d)

        two = total > whole
        head = jnp.where(two, (total + 1) // 2, total)

        def step(i, _):
            n = jnp.where(i == 0, head, total - head)
            for v in range(1, whole + 1):
                pl.when(n == v)(lambda v=v: part(i * head, v))
            return 0

        lax.fori_loop(0, jnp.where(two, 2, 1), step, 0)

        @pl.when(f == nf - 1)
        def _():
            for grp in range(groups):
                o = acc[pl.ds(0 if grp == 0 else lead, chunks)]
                out_ref[0, grp] = o.astype(jnp.bfloat16).reshape(chunks, 4, CHUNK, d)

    total = experts * groups * chunks * rows
    return pl.pallas_call(
        kern,
        out_shape=jax.ShapeDtypeStruct((experts, groups, chunks, 4, CHUNK, d), jnp.bfloat16),
        grid_spec=pltpu.PrefetchScalarGridSpec(
            num_scalar_prefetch=2,
            grid=(experts, nf),
            in_specs=[
                pl.BlockSpec(codes.shape, lambda e, f, p, u: (0, 0, 0)),
                pl.BlockSpec(x.shape, lambda e, f, p, u: (0, 0), pipeline_mode=pl.Buffered(1)),
                pl.BlockSpec(
                    xs.shape, lambda e, f, p, u: (0, 0, 0), pipeline_mode=pl.Buffered(1)
                ),
                pl.BlockSpec((1, d, bf), lambda e, f, p, u: (p[e], 0, f)),
                pl.BlockSpec((1, d, bf), lambda e, f, p, u: (p[e], 0, f)),
                pl.BlockSpec((1, bf, d), lambda e, f, p, u: (p[e], f, 0)),
            ],
            out_specs=pl.BlockSpec(
                (1, groups, chunks, 4, CHUNK, d), lambda e, f, p, u: (e, 0, 0, 0, 0, 0)
            ),
            scratch_shapes=[
                pltpu.VMEM((groups * chunks, 4, CHUNK, d), jnp.bfloat16),
                pltpu.VMEM((groups * chunks, rows, d), jnp.float32),
            ],
        ),
        compiler_params=params(2),
        cost_estimate=pl.CostEstimate(
            flops=4 * total * d * ff,
            bytes_accessed=6 * experts * d * ff,
            transcendentals=total * ff,
        ),
        name="routed",
    )(picked, used, codes, x, xs, wg, wu, wd)


def solution(mesh):
    def body(x, expert, slot, gate, wg, wu, wd, sg, su, sd):
        x = x[0, 0]
        tokens = x.shape[0]
        top, ff = expert.shape[-1], sg.shape[1]
        slots = 5 * tokens * top // (4 * wg.shape[0] * mesh.shape["ep"])
        me, part = lax.axis_index("ep"), lax.axis_index("dp")
        bf = 512
        blocks = ff // 2 // bf
        early, relay = 16, 10

        code = jnp.where(slot < slots, expert * slots + slot, -1)[0, 0]
        weight = gate[0, 0].astype(jnp.bfloat16).astype(jnp.float32)
        small = jnp.stack([code.astype(jnp.float32).T, weight.T])
        h, xs, smalls = gather_up(x, small, sg, su, blocks, early, relay, bf)
        base = jnp.reshape(me * wg.shape[0] * slots, (1,)).astype(jnp.int32)
        mine = jnp.reshape(part, (1,)).astype(jnp.int32)
        codes, gates, picked, used = plan_call(small, smalls, base, mine, slots)
        out = routed_call(x, xs, codes, picked, used, wg, wu, wd, slots, 512)
        y = reduce_up_down(x, xs, h, out, codes, gates, sg, su, sd, slots, bf)
        return y[None, None]

    lead = P("dp", "ep", None, None)
    return jax.shard_map(
        body,
        mesh=mesh,
        in_specs=(lead,) * 4 + (P("ep", None, None),) * 3 + (P(None, None),) * 3,
        out_specs=lead,
        check_vma=False,
    )
```

```python
import jax
import jax.numpy as jnp
from jax import lax
from jax.experimental import pallas as pl
from jax.experimental.pallas import tpu as pltpu
from jax.sharding import PartitionSpec as P

CHUNK = 16
VMEM_LIMIT = 66_500_000
X, Y, CORE = 2, 4, 1


def dot(a, b):
    return jnp.dot(a, b, preferred_element_type=jnp.float32)


def swiglu(g, u):
    return (g * jax.nn.sigmoid(g) * u).astype(jnp.bfloat16)


def params(n):
    return pltpu.CompilerParams(
        vmem_limit_bytes=VMEM_LIMIT, dimension_semantics=("arbitrary",) * n
    )


def place():
    ep = lax.axis_index("ep")
    return lax.axis_index("dp"), ep // 2, ep % 2


def peer(bits):
    y, x, core = place()
    y = 1 - y if bits & Y else y
    x = 1 - x if bits & X else x
    core = 1 - core if bits & CORE else core
    return (y, x * 2 + core)


def gather_up(x, small, sg, su, per_core, blocks, relay, bf):
    tokens, d = x.shape
    half = tokens // 2

    def kern(x_ref, small_ref, g_ref, u_ref, h_ref, all_x, all_small, x2, local, send, recv):
        i = pl.program_id(0)

        def copy(n, src, dst, bits):
            return pltpu.make_async_remote_copy(
                src_ref=src,
                dst_ref=dst,
                send_sem=send.at[n],
                recv_sem=recv.at[n],
                device_id=peer(bits),
                device_id_type=pl.DeviceIdType.MESH,
            )

        def at(bits):
            return all_x.at[bits - 1]

        top, bottom = pl.ds(0, half), pl.ds(half, half)
        first = [copy(n, x_ref, at(b), b) for n, b in enumerate((CORE, X, Y))]
        second = [
            copy(3, at(Y).at[top], at(X | Y).at[top], X),
            copy(4, at(X).at[bottom], at(X | Y).at[bottom], Y),
            copy(5, at(X), at(X | CORE), CORE),
            copy(6, at(Y), at(Y | CORE), CORE),
        ]
        third = [copy(7, at(X | Y), at(X | Y | CORE), CORE)]
        little = [copy(7 + b, small_ref, all_small.at[b - 1], b) for b in range(1, 8)]

        def up(v):
            return swiglu(dot(v, g_ref[...]), dot(v, u_ref[...]))

        @pl.when(i == 0)
        def _():
            own = pltpu.make_async_copy(x_ref, x2.at[pl.ds(0, tokens)], local.at[0])
            own.start()
            barrier = pltpu.get_barrier_semaphore()
            for bits in range(1, 8):
                pl.semaphore_signal(
                    barrier, inc=1, device_id=peer(bits), device_id_type=pl.DeviceIdType.MESH
                )
            pl.semaphore_wait(barrier, 7)
            for c in little + first:
                c.start()
            own.wait()
            h_ref[:tokens] = up(x2[:tokens])
            first[0].wait_recv()
            other = pltpu.make_async_copy(at(CORE), x2.at[pl.ds(tokens, tokens)], local.at[1])
            other.start()
            other.wait()
            h_ref[tokens:] = up(x2[tokens:])

        @pl.when(i == relay)
        def _():
            first[1].wait_recv()
            first[2].wait_recv()
            for c in second:
                c.start()

        @pl.when(i == blocks - 1)
        def _():
            second[0].wait_recv()
            second[1].wait_recv()
            third[0].start()

        @pl.when(i > 0)
        def _():
            h_ref[...] = up(x2[...])

        @pl.when(i == blocks - 1)
        def _():
            second[2].wait_recv()
            second[3].wait_recv()
            for c in little:
                c.wait_recv()
            third[0].wait_recv()
            for c in first + second + third + little:
                c.wait_send()

    def column(i):
        return (0, (lax.axis_index("ep") % 2) * per_core + i)

    any_spec = pl.BlockSpec(memory_space=pl.ANY)
    return pl.pallas_call(
        kern,
        out_shape=[
            jax.ShapeDtypeStruct((2 * tokens, blocks * bf), jnp.bfloat16),
            jax.ShapeDtypeStruct((7, tokens, d), x.dtype),
            jax.ShapeDtypeStruct((7, *small.shape), small.dtype),
        ],
        grid=(blocks,),
        in_specs=[any_spec] * 2 + [pl.BlockSpec((d, bf), column)] * 2,
        out_specs=[pl.BlockSpec((2 * tokens, bf), lambda i: (0, i)), any_spec, any_spec],
        scratch_shapes=[
            pltpu.VMEM((2 * tokens, d), jnp.bfloat16),
            pltpu.SemaphoreType.DMA((2,)),
            pltpu.SemaphoreType.DMA((15,)),
            pltpu.SemaphoreType.DMA((15,)),
        ],
        compiler_params=pltpu.CompilerParams(
            vmem_limit_bytes=VMEM_LIMIT,
            dimension_semantics=("arbitrary",),
            collective_id=0,
            has_side_effects=True,
        ),
        cost_estimate=pl.CostEstimate(
            flops=8 * tokens * d * bf * blocks,
            bytes_accessed=4 * d * bf * blocks,
            transcendentals=2 * tokens * bf * blocks,
        ),
        name="gather_up",
    )(x, small, sg, su)


def reduce_up_down(x, xs, h, out, codes, gates, sg, su, sd, slots, bf):
    half, d = x.shape
    mid = half // 2
    experts, _, chunks = out.shape[:3]
    rows = experts * slots
    top = codes.shape[1]
    m, early = 2 * half, h.shape[1] // bf
    blocks = sd.shape[0] // 2 // bf
    late = blocks - early
    bu = bf // 2
    ups = 2 * late
    order = (7, 5, 3, 6, 1, 0)
    up0 = len(order)
    mid0 = up0 + ups
    down0 = mid0 + 2
    steps = down0 + blocks
    bn = 1792
    f32, bf16 = jnp.float32, jnp.bfloat16

    def kern(*refs):
        code_ref, gate_ref, x_ref, xs_ref, out_ref, g_ref, u_ref, h_ref, d_ref, y_ref = refs[:10]
        x2, hs, acc, weight, sends, cores, links, t_ref, b_ref, local, send, recv = refs[10:]
        i = pl.program_id(0)
        top_half, bottom = pl.ds(0, mid), pl.ds(mid, mid)
        own, other = pl.ds(0, half), pl.ds(half, half)
        moves = [
            (sends.at[0], cores.at[0], CORE),
            (sends.at[1], cores.at[1], CORE),
            (x2.at[other], cores.at[2], CORE),
            (sends.at[0].at[top_half], t_ref, Y),
            (sends.at[0].at[bottom], b_ref, X),
            (x2.at[own], links.at[0], X),
            (x2.at[other], links.at[1], Y),
            (sends.at[0], cores.at[3], CORE),
        ]
        copies = [
            pltpu.make_async_remote_copy(
                src_ref=src,
                dst_ref=dst,
                send_sem=send.at[n],
                recv_sem=recv.at[n],
                device_id=peer(bits),
                device_id_type=pl.DeviceIdType.MESH,
            )
            for n, (src, dst, bits) in enumerate(moves)
        ]
        loads = [
            pltpu.make_async_copy(x_ref, x2.at[own], local.at[0]),
            pltpu.make_async_copy(xs_ref.at[CORE - 1], x2.at[other], local.at[1]),
        ]

        def combine(s, put):
            row = lax.broadcasted_iota(jnp.int32, (rows, half), 0).astype(f32)
            w = jnp.zeros(row.shape, f32)
            for j in range(top):
                w = jnp.where(row == code_ref[s, j : j + 1, :], gate_ref[s, j : j + 1, :], w)
            weight[...] = w.T.astype(bf16)

            @pl.loop(0, d // bn)
            def _(n):
                cols = pl.ds(pl.multiple_of(n * bn, bn), bn)
                put(cols, dot(weight[...], out_ref[:, 0, :, 0, :, cols].reshape(rows, bn)))

        @pl.when(i == 0)
        def _():
            barrier = pltpu.get_barrier_semaphore()
            for bits in (CORE, X, Y):
                pl.semaphore_signal(
                    barrier, inc=1, device_id=peer(bits), device_id_type=pl.DeviceIdType.MESH
                )

        for n in range(3):

            @pl.when(i == n)
            def _(n=n):
                def put(cols, y):
                    if n < 2:
                        sends[n, :, cols] = y.astype(bf16)
                    else:
                        x2[other, cols] = y.astype(bf16)

                combine(order[n], put)
                if n == 0:
                    pl.semaphore_wait(pltpu.get_barrier_semaphore(), 3)
                copies[n].start()

        @pl.when(i == 3)
        def _():
            copies[0].wait_send()
            copies[0].wait_recv()

            def put(cols, y):
                sends[0, :, cols] = (y + cores[0, :, cols].astype(f32)).astype(bf16)

            combine(order[3], put)
            copies[3].start()
            copies[4].start()

        for n, where in ((4, other), (5, own)):

            @pl.when(i == n)
            def _(n=n, where=where):
                def put(cols, y):
                    acc[where, cols] = y

                if n == 5:
                    copies[2].wait_send()
                    for c in loads:
                        c.start()
                combine(order[n], put)
                if n == 5:
                    for c in loads:
                        c.wait()

        @pl.when((i >= up0) & (i < mid0))
        def _():
            hs[i - up0] = swiglu(dot(x2[...], g_ref[...]), dot(x2[...], u_ref[...]))

        @pl.when(i == mid0)
        def _():
            copies[2].wait_recv()
            copies[3].wait_recv()

            def put(cols, y):
                y = y + cores[2, :, cols].astype(f32)
                x2[top_half, cols] = (y[:mid] + t_ref[:, cols].astype(f32)).astype(bf16)
                x2[bottom, cols] = y[mid:].astype(bf16)

            combine(2, put)
            copies[5].start()

        @pl.when(i == mid0 + 1)
        def _():
            copies[1].wait_send()
            copies[1].wait_recv()
            copies[4].wait_recv()

            def put(cols, y):
                y = y + cores[1, :, cols].astype(f32)
                x2[pl.ds(half, mid), cols] = y[:mid].astype(bf16)
                x2[pl.ds(half + mid, mid), cols] = (
                    y[mid:] + b_ref[:, cols].astype(f32)
                ).astype(bf16)

            combine(4, put)
            copies[6].start()

        @pl.when((i >= down0) & (i < down0 + late))
        def _():
            j = 2 * (i - down0)
            acc[...] += dot(hs[j], d_ref[:bu]) + dot(hs[j + 1], d_ref[bu:])

        @pl.when(i >= down0 + late)
        def _():
            acc[...] += dot(h_ref[...], d_ref[...])

        @pl.when(i == steps - 1)
        def _():
            copies[3].wait_send()
            copies[4].wait_send()
            sends[0] = acc[other].astype(bf16)
            copies[7].start()
            copies[5].wait_recv()
            copies[6].wait_recv()
            acc[own] += links[0].astype(f32) + links[1].astype(f32)
            copies[7].wait_recv()
            sends[1] = (acc[own] + cores[3].astype(f32)).astype(bf16)
            result = pltpu.make_async_copy(sends.at[1], y_ref, local.at[0])
            result.start()
            for n in (5, 6, 7):
                copies[n].wait_send()
            result.wait()

    def core():
        return lax.axis_index("ep") % 2

    def source(i):
        s = jnp.where(i <= mid0, 2, 4)
        for n, v in enumerate(order):
            s = jnp.where(i == n, v, s)
        return (0, s // 4, 0, s % 4, 0, 0)

    def column(i):
        return (0, 2 * (core() * blocks + early) + jnp.clip(i - up0, 0, ups - 1))

    def down_row(i):
        j = jnp.maximum(i - down0, 0)
        return (core() * blocks + jnp.where(j < late, early + j, j - late), 0)

    any_spec = pl.BlockSpec(memory_space=pl.ANY)
    small_spec = pl.BlockSpec(codes.shape, lambda i: (0, 0, 0))
    dma = pltpu.SemaphoreType.DMA
    return pl.pallas_call(
        kern,
        out_shape=jax.ShapeDtypeStruct((half, d), bf16),
        grid=(steps,),
        in_specs=[small_spec, small_spec, any_spec, any_spec]
        + [pl.BlockSpec((experts, 1, chunks, 1, CHUNK, d), source)]
        + [pl.BlockSpec((d, bu), column)] * 2
        + [
            pl.BlockSpec((m, bf), lambda i: (0, jnp.maximum(i - down0 - late, 0))),
            pl.BlockSpec((bf, d), down_row),
        ],
        out_specs=any_spec,
        scratch_shapes=[
            pltpu.VMEM((m, d), bf16),
            pltpu.VMEM((ups, m, bu), bf16),
            pltpu.VMEM((m, d), f32),
            pltpu.VMEM((half, rows), bf16),
            pltpu.VMEM((2, half, d), bf16),
            pltpu.VMEM((4, half, d), bf16),
            pltpu.VMEM((2, half, d), bf16),
            pltpu.VMEM((mid, d), bf16),
            pltpu.VMEM((mid, d), bf16),
            dma((2,)),
            dma((8,)),
            dma((8,)),
        ],
        compiler_params=pltpu.CompilerParams(
            vmem_limit_bytes=VMEM_LIMIT,
            dimension_semantics=("arbitrary",),
            collective_id=1,
            has_side_effects=True,
        ),
        cost_estimate=pl.CostEstimate(
            flops=2 * m * d * bf * (blocks + 2 * late),
            bytes_accessed=2 * d * bf * (blocks + 2 * late),
            transcendentals=m * bf * late,
        ),
        name="reduce_up_down",
    )(codes, gates, x, xs, out, sg, su, h, sd)


def plan_call(small, smalls, base, part, slots):
    n_src, top, tokens = 1 + smalls.shape[0], *smalls.shape[2:]
    groups = n_src // 4
    experts = 4 * groups

    def kern(base_ref, part_ref, own_ref, small_ref, code_ref, gate_ref, expert_ref, used_ref):
        low = base_ref[0].astype(jnp.float32)
        codes = [own_ref[0] - low] + [small_ref[s, 0] - low for s in range(n_src - 1)]
        gate_ref[0] = own_ref[1]
        for s in range(1, n_src):
            gate_ref[s] = small_ref[s - 1, 1]
        used, total = [], []
        for e in range(experts):
            counts = []
            for grp in range(groups):
                most = jnp.full((top, tokens), -1.0, jnp.float32)
                for s in range(grp * 4, grp * 4 + 4):
                    here = (codes[s] >= e * slots) & (codes[s] < (e + 1) * slots)
                    most = jnp.maximum(most, jnp.where(here, codes[s] - e * slots, -1.0))
                counts.append((jnp.max(most).astype(jnp.int32) + CHUNK) // CHUNK)
            used.append(counts)
            total.append(sum(counts))
        news = [jnp.full((top, tokens), -1.0, jnp.float32) for _ in range(n_src)]
        for e in range(experts):
            rank = jnp.int32(0)
            for o in range(experts):
                if o != e:
                    ahead = total[o] >= total[e] if o < e else total[o] > total[e]
                    rank = rank + ahead.astype(jnp.int32)
            spot = rank // 2
            mine = (rank % 2 + spot % 2) % 2 == part_ref[0]

            @pl.when(mine)
            def _(e=e, spot=spot):
                expert_ref[spot] = e
                for grp in range(groups):
                    used_ref[spot, grp] = used[e][grp]

            shift = jnp.where(mine, (spot - e) * slots, -(10**6)).astype(jnp.float32)
            for s in range(n_src):
                here = (codes[s] >= e * slots) & (codes[s] < (e + 1) * slots)
                news[s] = jnp.where(here, codes[s] + shift, news[s])
        for s in range(n_src):
            code_ref[s] = news[s]

    smem = pl.BlockSpec(memory_space=pltpu.SMEM)
    vmem = pl.BlockSpec(memory_space=pltpu.VMEM)
    return pl.pallas_call(
        kern,
        out_shape=[jax.ShapeDtypeStruct((n_src, top, tokens), jnp.float32)] * 2
        + [
            jax.ShapeDtypeStruct((experts // groups,), jnp.int32),
            jax.ShapeDtypeStruct((experts // groups, groups), jnp.int32),
        ],
        in_specs=[smem, smem, vmem, vmem],
        out_specs=[vmem, vmem, smem, smem],
        name="plan",
    )(base, part, small, smalls)


def routed_call(x, xs, codes, picked, used, wg, wu, wd, slots, bf):
    n_src = 1 + xs.shape[0]
    groups = n_src // 4
    experts = picked.shape[0]
    d = x.shape[1]
    ff = wg.shape[2]
    nf = ff // bf
    chunks = slots // CHUNK
    top, tokens = codes.shape[1:]
    rows = 4 * CHUNK
    whole = 7
    wide = bf // 2

    def kern(picked_ref, used_ref, code_ref, x_ref, xs_ref, g_ref, u_ref, d_ref, out_ref, z, acc):
        e, f = pl.program_id(0), pl.program_id(1)
        lead = used_ref[e, 0]
        total = lead + used_ref[e, 1]

        @pl.when((e == 0) & (f == 0))
        def _():
            acc[...] = jnp.zeros_like(acc)

        @pl.when(f == 0)
        def _():
            low = (e * slots).astype(jnp.float32)
            row = low + lax.broadcasted_iota(jnp.int32, (slots, tokens), 0).astype(jnp.float32)
            for grp in range(groups):
                for k in range(4):
                    s = grp * 4 + k
                    pick = jnp.zeros((slots, tokens), jnp.float32)
                    for j in range(top):
                        pick = jnp.where(row == code_ref[s, j : j + 1, :], 1.0, pick)
                    pick = pick.astype(jnp.bfloat16)
                    zs = dot(pick, x_ref[...] if s == 0 else xs_ref[s - 1])
                    zs = zs.astype(jnp.bfloat16).reshape(chunks, CHUNK, d)
                    z[pl.ds(0 if grp == 0 else lead, chunks), k] = zs

        def part(first, n):
            m = n * rows
            zz = z[pl.ds(first, n)].reshape(m, d)
            h = jnp.concatenate(
                [
                    swiglu(dot(zz, g_ref[0, :, c : c + wide]), dot(zz, u_ref[0, :, c : c + wide]))
                    for c in range(0, bf, wide)
                ],
                axis=1,
            )
            old = jnp.where(f == 0, 0.0, acc[pl.ds(first, n)].reshape(m, d))
            acc[pl.ds(first, n)] = (old + dot(h, d_ref[0])).reshape(n, rows, d)

        two = total > whole
        head = jnp.where(two, (total + 1) // 2, total)

        def step(i, _):
            n = jnp.where(i == 0, head, total - head)
            for v in range(1, whole + 1):
                pl.when(n == v)(lambda v=v: part(i * head, v))
            return 0

        lax.fori_loop(0, jnp.where(two, 2, 1), step, 0)

        @pl.when(f == nf - 1)
        def _():
            for grp in range(groups):
                o = acc[pl.ds(0 if grp == 0 else lead, chunks)]
                out_ref[0, grp] = o.astype(jnp.bfloat16).reshape(chunks, 4, CHUNK, d)

    total = experts * groups * chunks * rows
    return pl.pallas_call(
        kern,
        out_shape=jax.ShapeDtypeStruct((experts, groups, chunks, 4, CHUNK, d), jnp.bfloat16),
        grid_spec=pltpu.PrefetchScalarGridSpec(
            num_scalar_prefetch=2,
            grid=(experts, nf),
            in_specs=[
                pl.BlockSpec(codes.shape, lambda e, f, p, u: (0, 0, 0)),
                pl.BlockSpec(x.shape, lambda e, f, p, u: (0, 0), pipeline_mode=pl.Buffered(1)),
                pl.BlockSpec(
                    xs.shape, lambda e, f, p, u: (0, 0, 0), pipeline_mode=pl.Buffered(1)
                ),
                pl.BlockSpec((1, d, bf), lambda e, f, p, u: (p[e], 0, f)),
                pl.BlockSpec((1, d, bf), lambda e, f, p, u: (p[e], 0, f)),
                pl.BlockSpec((1, bf, d), lambda e, f, p, u: (p[e], f, 0)),
            ],
            out_specs=pl.BlockSpec(
                (1, groups, chunks, 4, CHUNK, d), lambda e, f, p, u: (e, 0, 0, 0, 0, 0)
            ),
            scratch_shapes=[
                pltpu.VMEM((groups * chunks, 4, CHUNK, d), jnp.bfloat16),
                pltpu.VMEM((groups * chunks, rows, d), jnp.float32),
            ],
        ),
        compiler_params=params(2),
        cost_estimate=pl.CostEstimate(
            flops=4 * total * d * ff,
            bytes_accessed=6 * experts * d * ff,
            transcendentals=total * ff,
        ),
        name="routed",
    )(picked, used, codes, x, xs, wg, wu, wd)


def solution(mesh):
    def body(x, expert, slot, gate, wg, wu, wd, sg, su, sd):
        x = x[0, 0]
        tokens = x.shape[0]
        top, ff = expert.shape[-1], sg.shape[1]
        slots = 5 * tokens * top // (4 * wg.shape[0] * mesh.shape["ep"])
        me, part = lax.axis_index("ep"), lax.axis_index("dp")
        bf = 512
        blocks = ff // 2 // bf
        early, relay = 16, 10

        code = jnp.where(slot < slots, expert * slots + slot, -1)[0, 0]
        weight = gate[0, 0].astype(jnp.bfloat16).astype(jnp.float32)
        small = jnp.stack([code.astype(jnp.float32).T, weight.T])
        h, xs, smalls = gather_up(x, small, sg, su, blocks, early, relay, bf)
        base = jnp.reshape(me * wg.shape[0] * slots, (1,)).astype(jnp.int32)
        mine = jnp.reshape(part, (1,)).astype(jnp.int32)
        codes, gates, picked, used = plan_call(small, smalls, base, mine, slots)
        out = routed_call(x, xs, codes, picked, used, wg, wu, wd, slots, 512)
        y = reduce_up_down(x, xs, h, out, codes, gates, sg, su, sd, slots, bf)
        return y[None, None]

    lead = P("dp", "ep", None, None)
    return jax.shard_map(
        body,
        mesh=mesh,
        in_specs=(lead,) * 4 + (P("ep", None, None),) * 3 + (P(None, None),) * 3,
        out_specs=lead,
        check_vma=False,
    )
```
